256 devices in a mesh: gx: 8 (over y, core), gy: 4 (over x), gz: 8 (over z).
Axes of the slice: x: 4, y: 4, z: 8, core: 2. Of those that a mesh axis runs over, the one named last changes fastest.
Arguments:
- velocity: float32 [128, 64, 3, 1024], P('gx', 'gy', None, 'gz'), may hold values from -6 to 6
- marker_pos: float32 [16384, 3, 256], P(('gx', 'gy', 'gz')), may hold values from -130 to 256
- marker_force: float32 [16384, 3, 256], P(('gx', 'gy', 'gz')), may hold values from -6 to 6
- intersect: int32 [16384, 27], P(('gx', 'gy', 'gz')), may hold values from 0 to 1, as said below
- tiles: int32 [16384, 27, 16], P(('gx', 'gy', 'gz')), may hold values from 0 to 255, as said below
Outputs:
- velocity_out: float32 [128, 64, 3, 1024], P('gx', 'gy', None, 'gz')
- marker_velocity: float32 [16384, 3, 256], P(('gx', 'gy', 'gz'))
The draws below stay inside these ranges and needn't reach their ends.
Inputs may be any that keep to these rules, and one draw needn't show every extreme that they name: `intersect`: column 13 is always 1. Of one owner's bubbles at most 16 have a 1 in any other column; on every draw some owner has exactly 16 in some column, and some device is intersected by exactly 16 bubbles of its neighbour at each of the 26 other offsets. tiles[b, q, j] is a tile of the device at offset q from b's owner, numbered ix * 16 + iy for the line of cells (ix, iy); entries of columns where intersect is 0 are not used.
All inputs are finite; a program needn't handle non-finite values.
Results may differ from the reference program's by a relative error of at most 0.0049.
Values sent between devices are 32-bit elements; how exact they have to be, the bound alone decides.
A program may use at most 128 MiB of HBM per device.

```python
import math
import jax
import jax.numpy as jnp
import numpy as np
from jax import lax

CX = 16
CY = 16
TILE_LEN = 128
MARKERS = 256
BUB_DEV = 64
CAP = 16
TOUCH = 16
BUBBLES = 16384
NX = 128
NY = 64
NZ = 1024
N_GX = 8
N_GY = 4
N_GZ = 8
DEVICES = 256


def direction_offsets():
    direction = jnp.arange(27, dtype=jnp.int32)
    return (direction // 9 - 1, direction // 3 % 3 - 1, direction % 3 - 1)


def intersect_table(key):
    base_key = jax.random.fold_in(key, 7001)
    key_heavy, key_pick, key_count, key_score = jax.random.split(base_key, 4)
    device = jnp.arange(DEVICES, dtype=jnp.int32)
    heavy_recv = (jax.random.randint(key_heavy, (DEVICES,), 0, 4) == 0) | (device == jax.random.randint(key_pick, (), 0, DEVICES))
    light_counts = jax.random.randint(key_count, (DEVICES, 27), 1, max(CAP // 2, 1) + 1)
    recv_counts = jnp.where(heavy_recv[:, None], CAP, light_counts)
    off_x, off_y, off_z = direction_offsets()
    dev_x = device // (N_GY * N_GZ)
    dev_y = device // N_GZ % N_GY
    dev_z = device % N_GZ
    recv_x = (dev_x[:, None] + off_x[None, :]) % N_GX
    recv_y = (dev_y[:, None] + off_y[None, :]) % N_GY
    recv_z = (dev_z[:, None] + off_z[None, :]) % N_GZ
    receiver = (recv_x * N_GY + recv_y) * N_GZ + recv_z
    send_counts = recv_counts[receiver, jnp.arange(27, dtype=jnp.int32)[None, :]]
    scores = jax.random.randint(key_score, (DEVICES, 27, BUB_DEV), 0, 1 << 20) * BUB_DEV + jnp.arange(BUB_DEV, dtype=jnp.int32)
    ranking = jnp.sum((scores[:, :, None, :] < scores[:, :, :, None]).astype(jnp.int32), axis=3)
    chosen = (ranking < send_counts[:, :, None]) | (jnp.arange(27, dtype=jnp.int32)[None, :, None] == 13)
    return jnp.transpose(chosen, (0, 2, 1)).reshape(BUBBLES, 27).astype(jnp.int32)


def tile_table(key):
    base_key = jax.random.fold_in(key, 7002)
    key_cx, key_cy, key_cells = jax.random.split(base_key, 3)
    side = math.isqrt(max(TOUCH - 1, 0)) + 1
    window = min(CX, CY, 2 * side)
    corner_x = jax.random.randint(key_cx, (BUBBLES, 27, 1), 0, CX - window + 1)
    corner_y = jax.random.randint(key_cy, (BUBBLES, 27, 1), 0, CY - window + 1)
    scores = jax.random.randint(key_cells, (BUBBLES, 27, window * window), 0, 1 << 20) * (window * window) + jnp.arange(window * window, dtype=jnp.int32)
    _, cells = lax.top_k(scores, TOUCH)
    cells = cells.astype(jnp.int32)
    return ((corner_x + cells // window) * CY + corner_y + cells % window).astype(jnp.int32)


def draw_intersect(key, part):
    return intersect_table(key)


def draw_tiles(key, part):
    return tile_table(key)


def draw_marker_pos(key, part):
    tile_ids = tile_table(key)
    flags = intersect_table(key)
    anchor_key = jax.random.fold_in(key, 7004)
    key_code, key_slot = jax.random.split(anchor_key, 2)
    count = jnp.sum(flags, axis=1)
    pick = jax.random.randint(key_code, (BUBBLES, MARKERS), 0, count[:, None])
    running = jnp.cumsum(flags, axis=1)
    anchor_dir = jnp.zeros((BUBBLES, MARKERS), jnp.int32)
    for code in range(27):
        anchor_dir = anchor_dir + (running[:, code, None] <= pick).astype(jnp.int32)
    anchor_slot = jax.random.randint(key_slot, (BUBBLES, MARKERS), 0, TOUCH)
    flat_tiles = tile_ids.reshape(BUBBLES, 27 * TOUCH)
    anchored = jnp.take_along_axis(flat_tiles, anchor_dir * TOUCH + anchor_slot, axis=1)
    off_x, off_y, off_z = direction_offsets()
    jitter_key = jax.random.fold_in(key, 7003)
    key_x, key_y, key_z = jax.random.split(jitter_key, 3)
    jitter_width = 1.5
    shape_one = (BUBBLES, MARKERS)
    pos_x = (off_x[anchor_dir] * CX + anchored // CY).astype(jnp.float32) + jax.random.uniform(key_x, shape_one, jnp.float32, -jitter_width, jitter_width)
    pos_y = (off_y[anchor_dir] * CY + anchored % CY).astype(jnp.float32) + jax.random.uniform(key_y, shape_one, jnp.float32, -jitter_width, jitter_width)
    pos_z = (off_z[anchor_dir] * TILE_LEN).astype(jnp.float32) + jax.random.uniform(key_z, shape_one, jnp.float32, 0.0, float(TILE_LEN))
    return jnp.stack([pos_x, pos_y, pos_z], axis=1)


def steps_of(stream_key, extent, cuts, least, top_value):
    def one(dim, blocks):
        steps = jax.random.uniform(jax.random.fold_in(jax.random.fold_in(stream_key, 6), dim), (blocks,), jnp.float32, least / len(cuts), top_value / len(cuts))
        return jnp.repeat(jnp.exp(steps), extent[dim] // blocks).reshape((-1,) + (1,) * (len(extent) - dim - 1))

    factor_of = one(*cuts[0])
    for cut in cuts[1:]:
        factor_of = factor_of * one(*cut)
    return factor_of


def scatter_about(rng, shape, scale, most, cuts=(), kind=jnp.bfloat16):
    result = scale * jax.random.normal(rng, shape, jnp.float32)
    if cuts:
        result = result * steps_of(rng, shape, cuts, -0.22, 0.18)
    return jnp.clip(result, -most, most).astype(kind)


def setup_inputs(seed: int = 0) -> dict:
    key_of = jax.random.split(jax.random.key(seed), 6)
    return {
        "velocity": scatter_about(key_of[0], (NX, NY, 3, NZ), 1.0, 6.0, ((0, 8), (1, 4), (3, 8)), jnp.float32),
        "marker_pos": draw_marker_pos(jax.random.fold_in(key_of[5], 71), 0),
        "marker_force": scatter_about(key_of[2], (BUBBLES, 3, MARKERS), 1.0, 6.0, ((0, 256),), jnp.float32),
        "intersect": draw_intersect(jax.random.fold_in(key_of[5], 71), 0),
        "tiles": draw_tiles(jax.random.fold_in(key_of[5], 71), 0),
    }


spread_width = 0.5
viscous = 0.1


def offset_table():
    direction = jnp.arange(27, dtype=jnp.int32)
    return jnp.stack([direction // 9 - 1, (direction // 3) % 3 - 1, direction % 3 - 1], axis=1)


def line_weights(rel_pos, tile_ids, size_y, tile_len):
    cell_z = jnp.arange(tile_len, dtype=jnp.int32).astype(jnp.float32)
    along_z = jnp.exp(-spread_width * jnp.square(cell_z[None, :, None] - rel_pos[:, 2, None, :])).astype(jnp.bfloat16)
    tile_x = (tile_ids // size_y).astype(jnp.float32)
    tile_y = (tile_ids % size_y).astype(jnp.float32)
    across = jnp.exp(-spread_width * (jnp.square(tile_x[:, :, None] - rel_pos[:, None, 0, :]) + jnp.square(tile_y[:, :, None] - rel_pos[:, None, 1, :])))
    across = jnp.where(tile_ids[:, :, None] >= 0, across, jnp.zeros_like(across))
    return along_z, across


def compact_all(flag_cols):
    ranking = jnp.cumsum(flag_cols, axis=1) - 1
    slot_ids = jnp.arange(CAP, dtype=jnp.int32)
    matches = (ranking[:, None, :, :] == slot_ids[None, :, None, None]) & (flag_cols[:, None, :, :] == 1)
    bubble = jnp.arange(BUB_DEV, dtype=jnp.int32)
    picked = jnp.sum(jnp.where(matches, bubble[None, None, :, None], 0), axis=2).astype(jnp.int32)
    return picked, jnp.any(matches, axis=2)


def receiver_rows(device, marker_pos, marker_force, tiles, picked, usable):
    others = jnp.asarray(np.concatenate([np.arange(13), np.arange(14, 27)]), dtype=jnp.int32)
    offsets = offset_table()[others]
    here_at = jnp.stack([device // (N_GY * N_GZ), (device // N_GZ) % N_GY, device % N_GZ])
    mesh_sizes = jnp.array([N_GX, N_GY, N_GZ], dtype=jnp.int32)
    owner_at = (here_at[None, :] - offsets) % mesh_sizes[None, :]
    owners = ((owner_at[:, 0] * N_GY + owner_at[:, 1]) * N_GZ + owner_at[:, 2]).astype(jnp.int32)
    slot_ids = jnp.arange(CAP, dtype=jnp.int32)
    chosen = picked[owners[:, None], slot_ids[None, :], others[:, None]]
    is_valid = usable[owners[:, None], slot_ids[None, :], others[:, None]]
    global_id = (owners[:, None] * BUB_DEV + chosen).astype(jnp.int32)
    block_size = jnp.array([CX, CY, TILE_LEN], dtype=jnp.float32)
    shifts = offsets.astype(jnp.float32) * block_size[None, :]
    near_pos = marker_pos[global_id] - shifts[:, None, :, None]
    near_force = marker_force[global_id]
    near_tiles = jnp.where(is_valid[:, :, None], tiles[global_id, others[:, None]], -1)
    start = (device * BUB_DEV).astype(jnp.int32)
    own_pos = lax.dynamic_slice_in_dim(marker_pos, start, BUB_DEV, 0)
    own_force = lax.dynamic_slice_in_dim(marker_force, start, BUB_DEV, 0)
    own_tiles = lax.dynamic_slice_in_dim(tiles[:, 13, :], start, BUB_DEV, 0)
    rel_pos = jnp.concatenate([own_pos, near_pos.reshape(-1, 3, MARKERS)], axis=0)
    forces = jnp.concatenate([own_force, near_force.reshape(-1, 3, MARKERS)], axis=0)
    tile_ids = jnp.concatenate([own_tiles, near_tiles.reshape(-1, TOUCH)], axis=0).astype(jnp.int32)
    row_id = jnp.concatenate([start + jnp.arange(BUB_DEV, dtype=jnp.int32), global_id.reshape(-1)], axis=0).astype(jnp.int32)
    row_ok = jnp.concatenate([jnp.ones((BUB_DEV,), dtype=bool), is_valid.reshape(-1)], axis=0)
    return rel_pos, forces, tile_ids, row_id, row_ok


def reference(velocity, marker_pos, marker_force, intersect, tiles):
    flag_cols = intersect.reshape(DEVICES, BUB_DEV, 27)
    picked, usable = compact_all(flag_cols)
    usable = usable & (jnp.arange(27, dtype=jnp.int32)[None, None, :] != 13)
    tile_total = CX * CY

    def spread_one(device):
        rel_pos, forces, tile_ids, row_id, row_ok = receiver_rows(device, marker_pos, marker_force, tiles, picked, usable)
        along_z, across = line_weights(rel_pos, tile_ids, CY, TILE_LEN)
        scaled = (forces[:, None, :, :] * across[:, :, None, :]).astype(jnp.bfloat16)
        pieces = jnp.einsum("rtkm,rcm->rtkc", scaled.astype(jnp.float32), along_z.astype(jnp.float32), precision=lax.Precision.HIGHEST)
        target = jnp.where(tile_ids >= 0, tile_ids, tile_total).reshape(-1)
        summed = jax.ops.segment_sum(pieces.reshape(-1, 3, TILE_LEN), target, num_segments=tile_total + 1)
        return summed[:tile_total]

    forces_all = lax.map(spread_one, jnp.arange(DEVICES, dtype=jnp.int32))
    force_grid = forces_all.reshape(N_GX, N_GY, N_GZ, CX, CY, 3, TILE_LEN).transpose(0, 3, 1, 4, 5, 2, 6).reshape(CX * N_GX, CY * N_GY, 3, TILE_LEN * N_GZ)
    laplace = (jnp.roll(velocity, 1, 0) + jnp.roll(velocity, -1, 0) + jnp.roll(velocity, 1, 1) + jnp.roll(velocity, -1, 1)
               + jnp.roll(velocity, 1, 3) + jnp.roll(velocity, -1, 3) - 6.0 * velocity)
    velocity_out = velocity + viscous * laplace + force_grid
    grid_blocks = velocity_out.reshape(N_GX, CX, N_GY, CY, 3, N_GZ, TILE_LEN).transpose(0, 2, 5, 1, 3, 4, 6).reshape(DEVICES, tile_total, 3, TILE_LEN)

    def sample_one(running, device):
        rel_pos, forces, tile_ids, row_id, row_ok = receiver_rows(device, marker_pos, marker_force, tiles, picked, usable)
        along_z, across = line_weights(rel_pos, tile_ids, CY, TILE_LEN)
        grid_tiles = lax.dynamic_index_in_dim(grid_blocks, device, 0, keepdims=False)
        local_u = jnp.take(grid_tiles, jnp.maximum(tile_ids, 0), axis=0).astype(jnp.bfloat16)
        sampled = jnp.einsum("rtkc,rcm->rtkm", local_u.astype(jnp.float32), along_z.astype(jnp.float32), precision=lax.Precision.HIGHEST)
        partial_value = jnp.sum(sampled * across[:, :, None, :], axis=1)
        partial_value = jnp.where(row_ok[:, None, None], partial_value, jnp.zeros_like(partial_value))
        return running.at[row_id].add(partial_value), None

    marker_velocity, _ = lax.scan(sample_one, jnp.zeros((DEVICES * BUB_DEV, 3, MARKERS), jnp.float32), jnp.arange(DEVICES, dtype=jnp.int32))
    return velocity_out, marker_velocity
```

```python
import functools

import jax
import jax.numpy as jnp
from jax import lax
from jax.experimental import pallas as pl
from jax.experimental.pallas import tpu as pltpu
from jax.sharding import PartitionSpec as P

MESH = pl.DeviceIdType.MESH
CAP = 16
NEAR = 26
CHUNKS = 30
STEP = 5
LOG2E = 1.4426950408889634
ROOT = (0.5 * LOG2E) ** 0.5
F32 = jnp.float32
BF16 = jnp.bfloat16


def code_of(chunk):
    return (13 + STEP * jnp.minimum(chunk + 1, 27)) % 27


def offsets_of(chunk):
    code = code_of(chunk)
    return code // 9 - 1, code // 3 % 3 - 1, code % 3 - 1


def static_offsets(chunk):
    code = (13 + STEP * min(chunk + 1, 27)) % 27
    return code // 9 - 1, code // 3 % 3 - 1, code % 3 - 1


def iota(shape, dim):
    return lax.broadcasted_iota(jnp.int32, shape, dim)


def dot(a, b):
    return jnp.dot(a, b, preferred_element_type=F32)


def dot_nt(a, b):
    return lax.dot_general(a, b, (((1,), (1,)), ((), ())), preferred_element_type=F32)


def parts3(value):
    high = value.astype(BF16)
    rest = value - high.astype(F32)
    mid = rest.astype(BF16)
    low = (rest - mid.astype(F32)).astype(BF16)
    return jnp.concatenate([high, mid, low], axis=0)


def kernel(
    sizes, vel_ref, pos_ref, force_ref, flag_ref, tile_ref, grid_ref, out_ref,
    send, recv, along, across, picks, gather_t, scaled, pieces, low_grid, local_u, ret_send, ret_recv,
    face_y_send, face_z_send, face_x, face_y, face_z,
    send_sem, recv_sem, rsend_sem, rrecv_sem, hsend_sem, hrecv_sem,
):
    names = ("gx", "gy", "gz")
    me = [lax.axis_index(name) for name in names]
    around = [
        {d: lax.rem(at + (d + size), size) for d in (-1, 0, 1)} for at, size in zip(me, sizes)
    ]

    def near(offset):
        return tuple(around[i][offset[i]] for i in range(3))

    barrier = pltpu.get_barrier_semaphore()
    for n in range(NEAR):
        pl.semaphore_signal(barrier, inc=1, device_id=near(static_offsets(n)), device_id_type=MESH)

    rows = CHUNKS * CAP
    flags = flag_ref[...].astype(F32)
    before = (iota((64, 64), 0) <= iota((64, 64), 1)).astype(F32).astype(BF16)
    ranks = dot(flags.astype(BF16), before) - 1.0
    value = jnp.where(flags > 0.5, ranks, -1.0)
    value = jnp.concatenate([value, value, value], axis=1)
    row_chunk = iota((rows, 27), 0) // CAP
    chooser = (code_of(row_chunk) == iota((rows, 27), 1)).astype(F32).astype(BF16)
    row_value = dot(chooser, value.astype(BF16))
    own_value = (iota((rows, 192), 1) % 64 - (iota((rows, 192), 0) // CAP - NEAR) * CAP).astype(F32)
    row_value = jnp.where(iota((rows, 192), 0) >= NEAR * CAP, own_value, row_value)
    chosen = jnp.where(row_value == (iota((rows, 192), 0) % CAP).astype(F32), 1.0, 0.0)
    pick = chosen.astype(BF16)
    for f in range(6):
        source = pos_ref[f] if f < 3 else force_ref[f - 3]
        got = dot(pick, parts3(source)).reshape(CHUNKS, CAP, 256)
        send[:, f * CAP : (f + 1) * CAP, :] = got[:NEAR]
        recv[NEAR:, f * CAP : (f + 1) * CAP, :] = got[NEAR:]
    ids = (tile_ref[...].reshape(27 * CAP, 64) + 1).astype(F32).astype(BF16)
    all_ids = dot_nt(pick[:, :64], ids)
    same = code_of(iota((rows, 27 * CAP), 0) // CAP) == iota((rows, 27 * CAP), 1) // CAP
    all_ids = jnp.where(same, all_ids, 0.0).astype(BF16)
    spread_ids = (iota((27 * CAP, 256), 0) % CAP == iota((27 * CAP, 256), 1) % CAP).astype(F32).astype(BF16)
    wide = dot(all_ids, spread_ids)
    wide = jnp.where(iota((rows, 256), 0) % CAP == iota((rows, 256), 1) // CAP, wide, 0.0)
    id_rows = jnp.sum(wide.reshape(CHUNKS, CAP, 256), axis=1, keepdims=True) - 1.0
    id_rows = jnp.broadcast_to(id_rows, (CHUNKS, 8, 256))
    send[:, 96:104, :] = id_rows[:NEAR]
    recv[NEAR:, 96:104, :] = id_rows[NEAR:]

    last_row = (iota((CAP, 256), 1) == iota((CAP, 256), 0) * CAP + 15).astype(F32)
    first_row = (iota((CAP, 256), 1) == iota((CAP, 256), 0) * CAP).astype(F32)
    z_low, z_high = [], []
    for k in range(3):
        plane = vel_ref[:, k].reshape(256, 128)
        turned = plane.T
        z_low.append(turned[0:1])
        z_high.append(turned[127:128])
        face_y_send[0, k] = jnp.dot(last_row, plane, precision=lax.Precision.HIGHEST, preferred_element_type=F32)
        face_y_send[1, k] = jnp.dot(first_row, plane, precision=lax.Precision.HIGHEST, preferred_element_type=F32)
    pad = [jnp.zeros((5, 256), F32)]
    face_z_send[0] = jnp.concatenate(z_high + pad, axis=0)
    face_z_send[1] = jnp.concatenate(z_low + pad, axis=0)

    def halo(index):
        axis, side = divmod(index, 2)
        offset = [0, 0, 0]
        offset[axis] = 1 - 2 * side
        source = (vel_ref.at[15 if side == 0 else 0], face_y_send.at[side], face_z_send.at[side])[axis]
        target = (face_x.at[side], face_y.at[side], face_z.at[side])[axis]
        return pltpu.make_async_remote_copy(
            src_ref=source, dst_ref=target, send_sem=hsend_sem.at[index], recv_sem=hrecv_sem.at[index],
            device_id=near(offset), device_id_type=MESH,
        )

    def forward(n, device):
        return pltpu.make_async_remote_copy(
            src_ref=send.at[n], dst_ref=recv.at[n], send_sem=send_sem.at[n], recv_sem=recv_sem.at[n],
            device_id=device, device_id_type=MESH,
        )

    def back(n, device):
        return pltpu.make_async_remote_copy(
            src_ref=ret_send.at[n], dst_ref=ret_recv.at[n], send_sem=rsend_sem.at[n], recv_sem=rrecv_sem.at[n],
            device_id=device, device_id_type=MESH,
        )

    pl.semaphore_wait(barrier, NEAR)
    halos = [halo(i) for i in range(6)]
    for copy in halos:
        copy.start()
    for n in range(NEAR):
        forward(n, near(static_offsets(n))).start()

    gather_t[...] = jnp.concatenate([chosen[:, :128], jnp.zeros((32, 128), F32)], axis=0).T.astype(BF16)

    tile_y = iota((256, 128), 0) % CAP
    lane = iota((256, 128), 1)
    for k in range(3):
        plane = vel_ref[:, k].reshape(256, 128)
        near_y = jnp.where(tile_y == 0, 0.0, pltpu.roll(plane, 1, 0)) + jnp.where(
            tile_y == 15, 0.0, pltpu.roll(plane, 255, 0)
        )
        near_z = jnp.where(lane == 0, 0.0, pltpu.roll(plane, 1, 1)) + jnp.where(
            lane == 127, 0.0, pltpu.roll(plane, 127, 1)
        )
        none = jnp.zeros((CAP, 128), F32)
        near_x = jnp.concatenate([none, plane[:240]], axis=0) + jnp.concatenate([plane[16:], none], axis=0)
        total = plane + 0.1 * (near_x + near_y + near_z - 6.0 * plane)
        grid_ref[:, k] = total.reshape(16, 16, 128)

    def spread(chunk):
        off_x, off_y, off_z = offsets_of(chunk)
        ids = recv[chunk, 96:97, :]
        column = jnp.broadcast_to(ids, (128, 256)).T
        tile_x = jnp.floor(column * 0.0625)
        tile_y = column - 16.0 * tile_x
        placing = jnp.where(iota((256, 256), 0).astype(F32) == ids, 1.0, 0.0).astype(BF16)
        half = iota((256, 128), 1).astype(F32)
        picks[chunk, :, 0:128] = jnp.where(column == half, 1.0, 0.0).astype(BF16)
        picks[chunk, :, 128:256] = jnp.where(column == half + 128.0, 1.0, 0.0).astype(BF16)
        x = (recv[chunk, 0:16, :] - (off_x * 16).astype(F32)) * ROOT
        y = (recv[chunk, 16:32, :] - (off_y * 16).astype(F32)) * ROOT
        z = (recv[chunk, 32:48, :] - (off_z * 128).astype(F32)) * ROOT
        forces = [recv[chunk, 48 + 16 * k : 64 + 16 * k, :] for k in range(3)]
        cell = iota((128, 256), 0).astype(F32) * ROOT
        for r in range(CAP):
            part = slice(r * 16, r * 16 + 16)
            tx = tile_x[part] * ROOT
            ty = tile_y[part] * ROOT
            there = column[part]
            dx = jnp.concatenate([tx, tx], axis=1) - x[r : r + 1]
            dy = jnp.concatenate([ty, ty], axis=1) - y[r : r + 1]
            weight = jnp.exp2(-(dx * dx + dy * dy))
            weight = jnp.where(jnp.concatenate([there, there], axis=1) >= 0.0, weight, 0.0)
            across[chunk, r] = weight
            for k in range(3):
                scaled[r, 16 * k : 16 * k + 16, :] = (forces[k][r : r + 1] * weight).astype(BF16)
            dz = cell - z[r : r + 1]
            line = jnp.exp2(-(dz * dz)).astype(BF16)
            along[chunk, r] = line
            piece = dot_nt(scaled[r], line)
            for k in range(3):
                pieces[part, 128 * k : 128 * k + 128] = piece[16 * k : 16 * k + 16].astype(BF16)
        added = dot(placing, pieces[...])
        for k in range(3):
            grid_ref[:, k] += added[:, 128 * k : 128 * k + 128].reshape(16, 16, 128)

    @pl.loop(NEAR, CHUNKS)
    def _(chunk):
        spread(chunk)

    for copy in halos:
        copy.wait()
    at_row0 = (iota((256, CAP), 0) == iota((256, CAP), 1) * CAP).astype(F32)
    at_row15 = (iota((256, CAP), 0) == iota((256, CAP), 1) * CAP + 15).astype(F32)
    for k in range(3):
        grid_ref[0, k] += 0.1 * face_x[0, k]
        grid_ref[15, k] += 0.1 * face_x[1, k]
        extra = jnp.dot(at_row0, face_y[0, k], precision=lax.Precision.HIGHEST, preferred_element_type=F32)
        extra += jnp.dot(at_row15, face_y[1, k], precision=lax.Precision.HIGHEST, preferred_element_type=F32)
        low = jnp.broadcast_to(face_z[0, k : k + 1, :], (128, 256)).T
        high = jnp.broadcast_to(face_z[1, k : k + 1, :], (128, 256)).T
        extra += jnp.where(lane == 0, low, 0.0) + jnp.where(lane == 127, high, 0.0)
        grid_ref[:, k] += 0.1 * extra.reshape(16, 16, 128)

    beside = near((1, 0, 0))

    @pl.loop(0, NEAR)
    def _(chunk):
        forward(chunk, beside).wait_recv()
        spread(chunk)

    for k in range(3):
        low_grid[:, 128 * k : 128 * k + 128] = grid_ref[:, k].reshape(256, 128).astype(BF16)

    def sample(chunk, result):
        u = dot(picks[chunk], low_grid[...]).astype(BF16)
        for k in range(3):
            local_u[:, 16 * k : 16 * k + 16, :] = u[:, 128 * k : 128 * k + 128].reshape(16, 16, 128)
        for r in range(CAP):
            got = dot(local_u[r], along[chunk, r])
            weight = across[chunk, r]
            for k in range(3):
                result[k, r : r + 1, :] = jnp.sum(got[16 * k : 16 * k + 16] * weight, axis=0, keepdims=True)

    def origin(chunk):
        offset = offsets_of(chunk)
        return tuple(lax.rem(me[i] - offset[i] + sizes[i], sizes[i]) for i in range(3))

    @pl.loop(0, NEAR)
    def _(chunk):
        sample(chunk, ret_send.at[chunk])
        back(chunk, origin(chunk)).start()

    @pl.loop(NEAR, CHUNKS)
    def _(chunk):
        sample(chunk, ret_recv.at[chunk])

    @pl.loop(0, NEAR)
    def _(chunk):
        forward(chunk, beside).wait_send()
        back(chunk, beside).wait()

    gather = gather_t[0:64, 0:rows]
    for k in range(3):
        terms = ret_recv[:, k].reshape(rows, 256)
        high = terms.astype(BF16)
        low = (terms - high.astype(F32)).astype(BF16)
        out_ref[k] = dot(gather, high) + dot(gather, low)


def body(sizes, velocity, marker_pos, marker_force, intersect, tiles):
    vmem = pl.BlockSpec(memory_space=pltpu.VMEM)
    dma = pltpu.SemaphoreType.DMA
    grid, markers = pl.pallas_call(
        functools.partial(kernel, sizes),
        out_shape=(
            jax.ShapeDtypeStruct((16, 3, 16, 128), F32),
            jax.ShapeDtypeStruct((3, 64, 256), F32),
        ),
        in_specs=[vmem] * 5,
        out_specs=(vmem, vmem),
        scratch_shapes=[
            pltpu.VMEM((NEAR, 104, 256), F32),
            pltpu.VMEM((CHUNKS, 104, 256), F32),
            pltpu.VMEM((CHUNKS, CAP, 128, 256), BF16),
            pltpu.VMEM((CHUNKS, CAP, CAP, 256), F32),
            pltpu.VMEM((CHUNKS, 256, 256), BF16),
            pltpu.VMEM((128, 512), BF16),
            pltpu.VMEM((CAP, 48, 256), BF16),
            pltpu.VMEM((256, 384), BF16),
            pltpu.VMEM((256, 384), BF16),
            pltpu.VMEM((CAP, 48, 128), BF16),
            pltpu.VMEM((NEAR, 3, CAP, 256), F32),
            pltpu.VMEM((CHUNKS, 3, CAP, 256), F32),
            pltpu.VMEM((2, 3, CAP, 128), F32),
            pltpu.VMEM((2, 8, 256), F32),
            pltpu.VMEM((2, 3, CAP, 128), F32),
            pltpu.VMEM((2, 3, CAP, 128), F32),
            pltpu.VMEM((2, 8, 256), F32),
            dma((NEAR,)),
            dma((NEAR,)),
            dma((NEAR,)),
            dma((NEAR,)),
            dma((6,)),
            dma((6,)),
        ],
        compiler_params=pltpu.CompilerParams(
            collective_id=0, has_side_effects=True, vmem_limit_bytes=67043328
        ),
    )(
        jnp.transpose(velocity, (0, 2, 1, 3)),
        jnp.transpose(marker_pos, (1, 0, 2)),
        jnp.transpose(marker_force, (1, 0, 2)),
        intersect.T,
        jnp.transpose(tiles, (1, 2, 0)),
    )
    return jnp.transpose(grid, (0, 2, 1, 3)), jnp.transpose(markers, (1, 0, 2))


def solution(mesh):
    sizes = tuple(mesh.shape[name] for name in ("gx", "gy", "gz"))
    placed = (
        P("gx", "gy", None, "gz"),
        P(("gx", "gy", "gz"), None, None),
        P(("gx", "gy", "gz"), None, None),
        P(("gx", "gy", "gz"), None),
        P(("gx", "gy", "gz"), None, None),
    )
    return jax.shard_map(
        functools.partial(body, sizes),
        mesh=mesh,
        in_specs=placed,
        out_specs=(P("gx", "gy", None, "gz"), P(("gx", "gy", "gz"), None, None)),
        check_vma=False,
    )
```

```python
import functools

import jax
import jax.numpy as jnp
from jax import lax
from jax.experimental import pallas as pl
from jax.experimental.pallas import tpu as pltpu
from jax.sharding import PartitionSpec as P

MESH = pl.DeviceIdType.MESH
CAP = 16
NEAR = 26
CHUNKS = 30
LOG2E = 1.4426950408889634
ROOT = (0.5 * LOG2E) ** 0.5
HALF = -0.5 * LOG2E
F32 = jnp.float32
BF16 = jnp.bfloat16


FACES = [(1, 0, 0), (0, 0, 1), (0, 1, 0), (-1, 0, 0), (0, 0, -1), (0, -1, 0)]
EDGES = [
    (1, 0, 1), (0, 1, -1), (-1, 1, 0), (0, -1, 1), (-1, 0, -1), (1, -1, 0),
    (1, 1, 0), (0, -1, -1), (-1, 0, 1), (0, 1, 1), (1, 0, -1), (-1, -1, 0),
]
CORNERS = [
    (1, 1, 1), (-1, -1, -1), (1, -1, 1), (-1, 1, -1), (-1, 1, 1), (1, -1, -1), (1, 1, -1), (-1, -1, 1),
]
ORDER = FACES + EDGES + CORNERS + [(0, 0, 0)] * 4
WORDS = [
    sum((13 + 9 * x + 3 * y + z) << (5 * i) for i, (x, y, z) in enumerate(ORDER[6 * w : 6 * w + 6]))
    for w in range(5)
]


def code_of(chunk):
    word = jnp.where(chunk < 6, WORDS[0], WORDS[1])
    word = jnp.where(chunk < 12, word, WORDS[2])
    word = jnp.where(chunk < 18, word, WORDS[3])
    word = jnp.where(chunk < 24, word, WORDS[4])
    return lax.shift_right_logical(word, 5 * (chunk % 6)) % 32


def offsets_of(chunk):
    code = code_of(chunk)
    return code // 9 - 1, code // 3 % 3 - 1, code % 3 - 1


def iota(shape, dim):
    return lax.broadcasted_iota(jnp.int32, shape, dim)


def dot(a, b):
    return jnp.dot(a, b, preferred_element_type=F32)


def dot_nt(a, b):
    return lax.dot_general(a, b, (((1,), (1,)), ((), ())), preferred_element_type=F32)


def onehot(index, ids):
    return jnp.where(index.astype(F32) == ids, 1.0, 0.0).astype(BF16)


def merged(values):
    row = iota((8, 256), 0)
    for width in (4, 2, 1):
        first = row % (2 * width) < width
        if width == 4:
            values = [
                jnp.where(first, a, b) + pltpu.roll(jnp.where(first, b, a), 4, 0)
                for a, b in zip(values[:4], values[4:])
            ]
        else:
            values = [
                jnp.where(first, a, b) + jnp.where(first, pltpu.roll(a, 8 - width, 0), pltpu.roll(b, width, 0))
                for a, b in zip(values[:width], values[width:])
            ]
    return values[0]


def parts3(value):
    high = value.astype(BF16)
    rest = value - high.astype(F32)
    mid = rest.astype(BF16)
    low = (rest - mid.astype(F32)).astype(BF16)
    return jnp.concatenate([high, mid, low], axis=0)


def kernel(
    sizes, vel_ref, pos_ref, force_ref, flag_ref, tile_ref, grid_ref, out_ref,
    send, recv, send_ids, recv_ids, along, across, picks, gather_t, pieces, low_grid, local_u, ret_send, ret_recv,
    face_y_send, face_z_send, face_x, face_y, face_z,
    round_sem, send_sem, recv_sem, isend_sem, irecv_sem, rsend_sem, rrecv_sem, hsend_sem, hrecv_sem,
):
    names = ("gx", "gy", "gz")
    me = [lax.axis_index(name) for name in names]
    around = [
        {d: lax.rem(at + (d + size), size) for d in (-1, 0, 1)} for at, size in zip(me, sizes)
    ]

    def near(offset):
        return tuple(around[i][offset[i]] for i in range(3))

    barrier = pltpu.get_barrier_semaphore()
    for face in FACES:
        pl.semaphore_signal(barrier, inc=1, device_id=near(face), device_id_type=MESH)

    rows = CHUNKS * CAP
    flags = flag_ref[...].astype(F32)
    before = (iota((64, 64), 0) <= iota((64, 64), 1)).astype(F32).astype(BF16)
    ranks = dot(flags.astype(BF16), before) - 1.0
    value = jnp.where(flags > 0.5, ranks, -1.0)
    value = jnp.concatenate([value, value, value], axis=1)
    row_chunk = iota((rows, 27), 0) // CAP
    chooser = (code_of(row_chunk) == iota((rows, 27), 1)).astype(F32).astype(BF16)
    row_value = dot(chooser, value.astype(BF16))
    own_value = (iota((rows, 192), 1) % 64 - (iota((rows, 192), 0) // CAP - NEAR) * CAP).astype(F32)
    row_value = jnp.where(iota((rows, 192), 0) >= NEAR * CAP, own_value, row_value)
    chosen = jnp.where(row_value == (iota((rows, 192), 0) % CAP).astype(F32), 1.0, 0.0)
    pick = chosen.astype(BF16)
    for f in range(6):
        source = pos_ref[f] if f < 3 else force_ref[f - 3]
        got = dot(pick, parts3(source)).reshape(CHUNKS, CAP, 256)
        send[:, f * CAP : (f + 1) * CAP, :] = got[:NEAR]
        recv[NEAR:, f * CAP : (f + 1) * CAP, :] = got[NEAR:]
    ids = (tile_ref[...].reshape(27 * CAP, 64) + 1).astype(F32).astype(BF16)
    all_ids = dot_nt(pick[:, :64], ids)
    same = code_of(iota((rows, 27 * CAP), 0) // CAP) == iota((rows, 27 * CAP), 1) // CAP
    all_ids = jnp.where(same, all_ids, 0.0).astype(BF16)
    spread_ids = (iota((27 * CAP, 256), 0) % CAP == iota((27 * CAP, 256), 1) % CAP).astype(F32).astype(BF16)
    wide = dot(all_ids, spread_ids)
    wide = jnp.where(iota((rows, 256), 0) % CAP == iota((rows, 256), 1) // CAP, wide, 0.0)
    id_rows = jnp.sum(wide.reshape(CHUNKS, CAP, 256), axis=1, keepdims=True) - 1.0
    send_ids[...] = id_rows[:NEAR]
    recv_ids[NEAR:] = id_rows[NEAR:]

    last_row = (iota((CAP, 256), 1) == iota((CAP, 256), 0) * CAP + 15).astype(F32)
    first_row = (iota((CAP, 256), 1) == iota((CAP, 256), 0) * CAP).astype(F32)
    z_low, z_high = [], []
    for k in range(3):
        plane = vel_ref[:, k].reshape(256, 128)
        turned = plane.T
        z_low.append(turned[0:1])
        z_high.append(turned[127:128])
        face_y_send[0, k] = jnp.dot(last_row, plane, precision=lax.Precision.HIGHEST, preferred_element_type=F32)
        face_y_send[1, k] = jnp.dot(first_row, plane, precision=lax.Precision.HIGHEST, preferred_element_type=F32)
    pad = [jnp.zeros((5, 256), F32)]
    face_z_send[0] = jnp.concatenate(z_high + pad, axis=0)
    face_z_send[1] = jnp.concatenate(z_low + pad, axis=0)

    def halo(index):
        axis, side = divmod(index, 2)
        offset = [0, 0, 0]
        offset[axis] = 1 - 2 * side
        source = (vel_ref.at[15 if side == 0 else 0], face_y_send.at[side], face_z_send.at[side])[axis]
        target = (face_x.at[side], face_y.at[side], face_z.at[side])[axis]
        return pltpu.make_async_remote_copy(
            src_ref=source, dst_ref=target, send_sem=hsend_sem.at[index], recv_sem=hrecv_sem.at[index],
            device_id=near(offset), device_id_type=MESH,
        )

    def forward(n, device):
        return pltpu.make_async_remote_copy(
            src_ref=send.at[n], dst_ref=recv.at[n], send_sem=send_sem.at[n], recv_sem=recv_sem.at[n],
            device_id=device, device_id_type=MESH,
        )

    def forward_ids(n, device):
        return pltpu.make_async_remote_copy(
            src_ref=send_ids.at[n], dst_ref=recv_ids.at[n], send_sem=isend_sem.at[n], recv_sem=irecv_sem.at[n],
            device_id=device, device_id_type=MESH,
        )

    def go(low, high):
        for n in range(low, high):
            forward_ids(n, near(ORDER[n])).start()
            forward(n, near(ORDER[n])).start()

    def tell(index):
        for face in FACES:
            pl.semaphore_signal(round_sem.at[index], inc=1, device_id=near(face), device_id_type=MESH)

    def back(n, device):
        return pltpu.make_async_remote_copy(
            src_ref=ret_send.at[n], dst_ref=ret_recv.at[n], send_sem=rsend_sem.at[n], recv_sem=rrecv_sem.at[n],
            device_id=device, device_id_type=MESH,
        )

    pl.semaphore_wait(barrier, 6)
    tell(0)
    halos = [halo(i) for i in range(6)]
    for copy in halos:
        copy.start()
    go(0, 6)

    gather_t[...] = jnp.concatenate([chosen[:, :128], jnp.zeros((32, 128), F32)], axis=0).T.astype(BF16)

    tile_y = iota((256, 128), 0) % CAP
    lane = iota((256, 128), 1)
    for k in range(3):
        plane = vel_ref[:, k].reshape(256, 128)
        near_y = jnp.where(tile_y == 0, 0.0, pltpu.roll(plane, 1, 0)) + jnp.where(
            tile_y == 15, 0.0, pltpu.roll(plane, 255, 0)
        )
        near_z = jnp.where(lane == 0, 0.0, pltpu.roll(plane, 1, 1)) + jnp.where(
            lane == 127, 0.0, pltpu.roll(plane, 127, 1)
        )
        none = jnp.zeros((CAP, 128), F32)
        near_x = jnp.concatenate([none, plane[:240]], axis=0) + jnp.concatenate([plane[16:], none], axis=0)
        total = 0.1 * (near_x + near_y + near_z - 6.0 * plane)
        grid_ref[:, k] = total.reshape(16, 16, 128)

    def spread(chunk):
        off_x, off_y, off_z = offsets_of(chunk)
        ids = recv_ids[chunk]
        column = jnp.broadcast_to(ids, (128, 256)).T
        tile_x = jnp.floor(column * 0.0625)
        tile_y = column - 16.0 * tile_x
        placing = onehot(iota((256, 256), 0), ids)
        picks[chunk, 0] = onehot(iota((256, 128), 1), column)
        picks[chunk, 1] = onehot(iota((256, 128), 1) + 128, column)
        x = (recv[chunk, 0:16, :] - (off_x * 16).astype(F32)) * ROOT
        y = (recv[chunk, 16:32, :] - (off_y * 16).astype(F32)) * ROOT
        z = recv[chunk, 32:48, :] - (off_z * 128).astype(F32) - 64.0
        forces = [recv[chunk, 48 + 16 * k : 64 + 16 * k, :] for k in range(3)]
        step = iota((8, 256), 0).astype(F32)
        for r in range(CAP):
            part = slice(r * 16, r * 16 + 16)
            tx = tile_x[part] * ROOT
            ty = tile_y[part] * ROOT
            there = column[part]
            dx = jnp.concatenate([tx, tx], axis=1) - x[r : r + 1]
            dy = jnp.concatenate([ty, ty], axis=1) - y[r : r + 1]
            weight = jnp.exp2(-(dx * dx + dy * dy))
            weight = jnp.where(jnp.concatenate([there, there], axis=1) >= 0.0, weight, 0.0)
            across[chunk, r] = weight
            scaled = jnp.concatenate([(forces[k][r : r + 1] * weight).astype(BF16) for k in range(3)], axis=0)
            dz = step - z[r : r + 1]
            lean = dz * (16.0 * HALF)
            start = dz * dz * HALF
            powers = {8: start}
            up, down = lean + 64.0 * HALF, 64.0 * HALF - lean
            at = start
            for g in range(9, 16):
                at = at + up
                powers[g] = at
                up = up + 128.0 * HALF
            at = start
            for g in range(7, -1, -1):
                at = at + down
                powers[g] = at
                down = down + 128.0 * HALF
            line = jnp.concatenate([jnp.exp2(powers[g]) for g in range(16)], axis=0).astype(BF16)
            along[chunk, r, 0] = line[:, :128]
            along[chunk, r, 1] = line[:, 128:]
            piece = dot_nt(scaled, line).astype(BF16)
            for k in range(3):
                pieces[k, part, :] = piece[16 * k : 16 * k + 16]
        added = dot(placing, jnp.concatenate([pieces[k] for k in range(3)], axis=1))
        for k in range(3):
            grid_ref[:, k] += added[:, 128 * k : 128 * k + 128].reshape(16, 16, 128)

    @pl.loop(NEAR, NEAR + 2)
    def _(chunk):
        spread(chunk)

    pl.semaphore_wait(round_sem.at[0], 6)
    tell(1)
    go(6, 18)

    @pl.loop(NEAR + 2, CHUNKS)
    def _(chunk):
        spread(chunk)

    pl.semaphore_wait(round_sem.at[1], 6)
    go(18, NEAR)

    for copy in halos:
        copy.wait()
    at_row0 = (iota((256, CAP), 0) == iota((256, CAP), 1) * CAP).astype(F32)
    at_row15 = (iota((256, CAP), 0) == iota((256, CAP), 1) * CAP + 15).astype(F32)
    for k in range(3):
        grid_ref[0, k] += 0.1 * face_x[0, k]
        grid_ref[15, k] += 0.1 * face_x[1, k]
        extra = jnp.dot(at_row0, face_y[0, k], precision=lax.Precision.HIGHEST, preferred_element_type=F32)
        extra += jnp.dot(at_row15, face_y[1, k], precision=lax.Precision.HIGHEST, preferred_element_type=F32)
        low = jnp.broadcast_to(face_z[0, k : k + 1, :], (128, 256)).T
        high = jnp.broadcast_to(face_z[1, k : k + 1, :], (128, 256)).T
        extra += jnp.where(lane == 0, low, 0.0) + jnp.where(lane == 127, high, 0.0)
        grid_ref[:, k] += 0.1 * extra.reshape(16, 16, 128)

    beside = near((1, 0, 0))

    @pl.loop(0, NEAR)
    def _(chunk):
        forward_ids(chunk, beside).wait_recv()
        forward(chunk, beside).wait_recv()
        spread(chunk)

    for k in range(3):
        low_grid[k] = (vel_ref[:, k] + grid_ref[:, k]).reshape(256, 128).astype(BF16)

    def sample(chunk, result):
        pick_rows = jnp.concatenate([picks[chunk, 0], picks[chunk, 1]], axis=1)
        u = dot(pick_rows, jnp.concatenate([low_grid[k] for k in range(3)], axis=1)).astype(BF16)
        for k in range(3):
            local_u[:, 16 * k : 16 * k + 16, :] = u[:, 128 * k : 128 * k + 128].reshape(16, 16, 128)
        for half in range(2):
            sums = [[], [], []]
            for r in range(8 * half, 8 * half + 8):
                line = jnp.concatenate([along[chunk, r, 0], along[chunk, r, 1]], axis=1)
                got = dot(local_u[r], line)
                weight = across[chunk, r]
                for k in range(3):
                    value = got[16 * k : 16 * k + 16] * weight
                    sums[k].append(value[0:8] + value[8:16])
            for k in range(3):
                result[k, 8 * half : 8 * half + 8, :] = merged(sums[k])

    def origin(chunk):
        offset = offsets_of(chunk)
        return tuple(lax.rem(me[i] - offset[i] + sizes[i], sizes[i]) for i in range(3))

    @pl.loop(0, NEAR)
    def _(turn):
        chunk = NEAR - 1 - turn
        sample(chunk, ret_send.at[chunk])
        back(chunk, origin(chunk)).start()

    @pl.loop(NEAR, CHUNKS)
    def _(chunk):
        sample(chunk, ret_recv.at[chunk])

    @pl.loop(0, NEAR)
    def _(chunk):
        forward_ids(chunk, beside).wait_send()
        forward(chunk, beside).wait_send()
        back(chunk, beside).wait()

    gather = gather_t[0:64, 0:rows]
    for k in range(3):
        terms = ret_recv[:, k].reshape(rows, 256)
        high = terms.astype(BF16)
        low = (terms - high.astype(F32)).astype(BF16)
        out_ref[k] = dot(gather, high) + dot(gather, low)


def body(sizes, velocity, marker_pos, marker_force, intersect, tiles):
    vmem = pl.BlockSpec(memory_space=pltpu.VMEM)
    dma = pltpu.SemaphoreType.DMA
    grid, markers = pl.pallas_call(
        functools.partial(kernel, sizes),
        out_shape=(
            jax.ShapeDtypeStruct((16, 3, 16, 128), F32),
            jax.ShapeDtypeStruct((3, 64, 256), F32),
        ),
        in_specs=[vmem] * 5,
        out_specs=(vmem, vmem),
        scratch_shapes=[
            pltpu.VMEM((NEAR, 96, 256), F32),
            pltpu.VMEM((CHUNKS, 96, 256), F32),
            pltpu.VMEM((NEAR, 1, 256), F32),
            pltpu.VMEM((CHUNKS, 1, 256), F32),
            pltpu.VMEM((CHUNKS, CAP, 2, 128, 128), BF16),
            pltpu.VMEM((CHUNKS, CAP, CAP, 256), F32),
            pltpu.VMEM((CHUNKS, 2, 256, 128), BF16),
            pltpu.VMEM((128, 512), BF16),
            pltpu.VMEM((3, 256, 128), BF16),
            pltpu.VMEM((3, 256, 128), BF16),
            pltpu.VMEM((CAP, 48, 128), BF16),
            pltpu.VMEM((NEAR, 3, CAP, 256), F32),
            pltpu.VMEM((CHUNKS, 3, CAP, 256), F32),
            pltpu.VMEM((2, 3, CAP, 128), F32),
            pltpu.VMEM((2, 8, 256), F32),
            pltpu.VMEM((2, 3, CAP, 128), F32),
            pltpu.VMEM((2, 3, CAP, 128), F32),
            pltpu.VMEM((2, 8, 256), F32),
            pltpu.SemaphoreType.REGULAR((2,)),
            dma((NEAR,)),
            dma((NEAR,)),
            dma((NEAR,)),
            dma((NEAR,)),
            dma((NEAR,)),
            dma((NEAR,)),
            dma((6,)),
            dma((6,)),
        ],
        compiler_params=pltpu.CompilerParams(
            collective_id=0, has_side_effects=True, vmem_limit_bytes=67043328
        ),
    )(
        jnp.transpose(velocity, (0, 2, 1, 3)),
        jnp.transpose(marker_pos, (1, 0, 2)),
        jnp.transpose(marker_force, (1, 0, 2)),
        intersect.T,
        jnp.transpose(tiles, (1, 2, 0)),
    )
    return velocity + jnp.transpose(grid, (0, 2, 1, 3)), jnp.transpose(markers, (1, 0, 2))


def solution(mesh):
    sizes = tuple(mesh.shape[name] for name in ("gx", "gy", "gz"))
    placed = (
        P("gx", "gy", None, "gz"),
        P(("gx", "gy", "gz"), None, None),
        P(("gx", "gy", "gz"), None, None),
        P(("gx", "gy", "gz"), None),
        P(("gx", "gy", "gz"), None, None),
    )
    return jax.shard_map(
        functools.partial(body, sizes),
        mesh=mesh,
        in_specs=placed,
        out_specs=(P("gx", "gy", None, "gz"), P(("gx", "gy", "gz"), None, None)),
        check_vma=False,
    )
```

```python
import functools

import jax
import jax.numpy as jnp
from jax import lax
from jax.experimental import pallas as pl
from jax.experimental.pallas import tpu as pltpu
from jax.sharding import PartitionSpec as P

MESH = pl.DeviceIdType.MESH
CAP = 16
NEAR = 26
CHUNKS = 30
LOG2E = 1.4426950408889634
ROOT = (0.5 * LOG2E) ** 0.5
HALF = -0.5 * LOG2E
F32 = jnp.float32
BF16 = jnp.bfloat16


FACES = [(1, 0, 0), (0, 0, 1), (0, 1, 0), (-1, 0, 0), (0, 0, -1), (0, -1, 0)]
EDGES = [
    (1, 0, 1), (0, 1, -1), (-1, 1, 0), (0, -1, 1), (-1, 0, -1), (1, -1, 0),
    (1, 1, 0), (0, -1, -1), (-1, 0, 1), (0, 1, 1), (1, 0, -1), (-1, -1, 0),
]
CORNERS = [
    (1, 1, 1), (-1, -1, -1), (1, -1, 1), (-1, 1, -1), (-1, 1, 1), (1, -1, -1), (1, 1, -1), (-1, -1, 1),
]
ORDER = FACES + EDGES + CORNERS + [(0, 0, 0)] * 4
WORDS = [
    sum((13 + 9 * x + 3 * y + z) << (5 * i) for i, (x, y, z) in enumerate(ORDER[6 * w : 6 * w + 6]))
    for w in range(5)
]


def code_of(chunk):
    word = jnp.where(chunk < 6, WORDS[0], WORDS[1])
    word = jnp.where(chunk < 12, word, WORDS[2])
    word = jnp.where(chunk < 18, word, WORDS[3])
    word = jnp.where(chunk < 24, word, WORDS[4])
    return lax.shift_right_logical(word, 5 * (chunk % 6)) % 32


def offsets_of(chunk):
    code = code_of(chunk)
    return code // 9 - 1, code // 3 % 3 - 1, code % 3 - 1


def iota(shape, dim):
    return lax.broadcasted_iota(jnp.int32, shape, dim)


def dot(a, b):
    return jnp.dot(a, b, preferred_element_type=F32)


def dot_nt(a, b):
    return lax.dot_general(a, b, (((1,), (1,)), ((), ())), preferred_element_type=F32)


def onehot(index, ids):
    return jnp.where(index.astype(F32) == ids, 1.0, 0.0).astype(BF16)


def merged(values):
    row = iota((8, 256), 0)
    for width in (4, 2, 1):
        first = row % (2 * width) < width
        if width == 4:
            values = [
                jnp.where(first, a, b) + pltpu.roll(jnp.where(first, b, a), 4, 0)
                for a, b in zip(values[:4], values[4:])
            ]
        else:
            values = [
                jnp.where(first, a, b) + jnp.where(first, pltpu.roll(a, 8 - width, 0), pltpu.roll(b, width, 0))
                for a, b in zip(values[:width], values[width:])
            ]
    return values[0]


def parts3(value):
    high = value.astype(BF16)
    rest = value - high.astype(F32)
    mid = rest.astype(BF16)
    low = (rest - mid.astype(F32)).astype(BF16)
    return jnp.concatenate([high, mid, low], axis=0)


def kernel(
    sizes, vel_in, pos_in, force_in, flag_in, tile_in, grid_ref, out_ref,
    vel_ref, pos_ref, force_ref, flag_ref, tile_ref, in_sem, split,
    send, recv, send_ids, recv_ids, along, across, picks, gather_t, pieces, low_grid, local_u, ret_send, ret_recv,
    face_y_send, face_z_send, face_x, face_y, face_z,
    round_sem, send_sem, recv_sem, isend_sem, irecv_sem, rsend_sem, rrecv_sem, hsend_sem, hrecv_sem,
):
    names = ("gx", "gy", "gz")
    me = [lax.axis_index(name) for name in names]
    around = [
        {d: lax.rem(at + (d + size), size) for d in (-1, 0, 1)} for at, size in zip(me, sizes)
    ]

    def near(offset):
        return tuple(around[i][offset[i]] for i in range(3))

    barrier = pltpu.get_barrier_semaphore()
    for face in FACES:
        pl.semaphore_signal(barrier, inc=1, device_id=near(face), device_id_type=MESH)

    loads = [
        pltpu.make_async_copy(source, target, in_sem.at[i])
        for i, (source, target) in enumerate(
            [(flag_in, flag_ref), (pos_in, pos_ref), (force_in, force_ref), (vel_in, vel_ref), (tile_in, tile_ref)]
        )
    ]
    for copy in loads:
        copy.start()

    def halo(index):
        axis, side = divmod(index, 2)
        offset = [0, 0, 0]
        offset[axis] = 1 - 2 * side
        source = (vel_ref.at[15 if side == 0 else 0], face_y_send.at[side], face_z_send.at[side])[axis]
        target = (face_x.at[side], face_y.at[side], face_z.at[side])[axis]
        return pltpu.make_async_remote_copy(
            src_ref=source, dst_ref=target, send_sem=hsend_sem.at[index], recv_sem=hrecv_sem.at[index],
            device_id=near(offset), device_id_type=MESH,
        )

    def forward(n, device):
        return pltpu.make_async_remote_copy(
            src_ref=send.at[n], dst_ref=recv.at[n], send_sem=send_sem.at[n], recv_sem=recv_sem.at[n],
            device_id=device, device_id_type=MESH,
        )

    def forward_ids(n, device):
        return pltpu.make_async_remote_copy(
            src_ref=send_ids.at[n], dst_ref=recv_ids.at[n], send_sem=isend_sem.at[n], recv_sem=irecv_sem.at[n],
            device_id=device, device_id_type=MESH,
        )

    def go(low, high):
        for n in range(low, high):
            forward(n, near(ORDER[n])).start()

    def go_ids(low, high):
        for n in range(low, high):
            forward_ids(n, near(ORDER[n])).start()

    def tell(index):
        for face in FACES:
            pl.semaphore_signal(round_sem.at[index], inc=1, device_id=near(face), device_id_type=MESH)

    def back(n, device):
        return pltpu.make_async_remote_copy(
            src_ref=ret_send.at[n], dst_ref=ret_recv.at[n], send_sem=rsend_sem.at[n], recv_sem=rrecv_sem.at[n],
            device_id=device, device_id_type=MESH,
        )

    loads[0].wait()
    flags = flag_ref[...].astype(F32)
    before = (iota((64, 64), 0) <= iota((64, 64), 1)).astype(F32).astype(BF16)
    ranks = dot(flags.astype(BF16), before) - 1.0
    value = jnp.where(flags > 0.5, ranks, -1.0)
    value = jnp.concatenate([value, value, value], axis=1).astype(BF16)
    lanes27 = iota((CAP, 27), 1)

    def code_rows(low, high):
        return jnp.concatenate(
            [jnp.where(lanes27 == 13 + 9 * x + 3 * y + z, 1.0, 0.0) for x, y, z in ORDER[low:high]], axis=0
        ).astype(BF16)

    def slot_rows(low, high):
        rows = (high - low) * CAP
        slot = (iota((rows, 192), 0) & 15).astype(F32)
        return jnp.where(dot(code_rows(low, high), value) == slot, 1.0, 0.0)

    face_pick = slot_rows(0, 6).astype(BF16)
    loads[1].wait()
    loads[2].wait()
    for f in range(6):
        split[f] = parts3(pos_ref[f] if f < 3 else force_ref[f - 3])
        send[0:6, f * CAP : (f + 1) * CAP, :] = dot(face_pick, split[f]).reshape(6, CAP, 256)

    pl.semaphore_wait(barrier, 6)
    tell(0)
    go(0, 6)

    loads[3].wait()
    last_row = (iota((CAP, 256), 1) == iota((CAP, 256), 0) * CAP + 15).astype(F32)
    first_row = (iota((CAP, 256), 1) == iota((CAP, 256), 0) * CAP).astype(F32)
    z_low, z_high = [], []
    for k in range(3):
        plane = vel_ref[:, k].reshape(256, 128)
        turned = plane.T
        z_low.append(turned[0:1])
        z_high.append(turned[127:128])
        face_y_send[0, k] = jnp.dot(last_row, plane, precision=lax.Precision.HIGHEST, preferred_element_type=F32)
        face_y_send[1, k] = jnp.dot(first_row, plane, precision=lax.Precision.HIGHEST, preferred_element_type=F32)
    pad = [jnp.zeros((5, 256), F32)]
    face_z_send[0] = jnp.concatenate(z_high + pad, axis=0)
    face_z_send[1] = jnp.concatenate(z_low + pad, axis=0)

    rest = slot_rows(6, NEAR)
    rest_pick = rest.astype(BF16)
    own_rows = jnp.where((iota((64, 192), 1) & 63) == iota((64, 192), 0), 1.0, 0.0)
    own_pick = own_rows.astype(BF16)
    for f in range(6):
        got = dot(jnp.concatenate([rest_pick, own_pick], axis=0), split[f]).reshape(CHUNKS - 6, CAP, 256)
        send[6:NEAR, f * CAP : (f + 1) * CAP, :] = got[: NEAR - 6]
        recv[NEAR:, f * CAP : (f + 1) * CAP, :] = got[NEAR - 6 :]
    halos = [halo(i) for i in range(6)]
    for copy in halos:
        copy.start()
    pl.semaphore_wait(round_sem.at[0], 6)
    tell(1)

    loads[4].wait()
    rows = CHUNKS * CAP
    pick = jnp.concatenate([face_pick, rest_pick, own_pick], axis=0)
    ids = (tile_ref[...].reshape(27 * CAP, 64) + 1).astype(F32).astype(BF16)
    all_ids = dot_nt(pick[:, :64], ids)
    each = jnp.where(iota((27, 27 * CAP), 0) == lax.shift_right_logical(iota((27, 27 * CAP), 1), 4), 1.0, 0.0)
    same = dot(code_rows(0, CHUNKS), each.astype(BF16))
    all_ids = (all_ids * same).astype(BF16)
    spread_ids = jnp.where((iota((27 * CAP, 256), 0) & 15) == (iota((27 * CAP, 256), 1) & 15), 1.0, 0.0).astype(BF16)
    wide = dot(all_ids, spread_ids)
    wide = jnp.where((iota((rows, 256), 0) & 15) == lax.shift_right_logical(iota((rows, 256), 1), 4), wide, 0.0)
    id_rows = jnp.sum(wide.reshape(CHUNKS, CAP, 256), axis=1, keepdims=True) - 1.0
    send_ids[...] = id_rows[:NEAR]
    recv_ids[NEAR:] = id_rows[NEAR:]
    go_ids(0, 18)
    go(6, 18)
    face_rows = slot_rows(0, 6)
    gather_t[...] = jnp.concatenate(
        [face_rows[:, :128], rest[:, :128], own_rows[:, :128], jnp.zeros((32, 128), F32)], axis=0
    ).T.astype(BF16)
    pl.semaphore_wait(round_sem.at[1], 6)
    go_ids(18, NEAR)
    go(18, NEAR)

    tile_y = iota((256, 128), 0) % CAP
    lane = iota((256, 128), 1)
    for k in range(3):
        plane = vel_ref[:, k].reshape(256, 128)
        near_y = jnp.where(tile_y == 0, 0.0, pltpu.roll(plane, 1, 0)) + jnp.where(
            tile_y == 15, 0.0, pltpu.roll(plane, 255, 0)
        )
        near_z = jnp.where(lane == 0, 0.0, pltpu.roll(plane, 1, 1)) + jnp.where(
            lane == 127, 0.0, pltpu.roll(plane, 127, 1)
        )
        none = jnp.zeros((CAP, 128), F32)
        near_x = jnp.concatenate([none, plane[:240]], axis=0) + jnp.concatenate([plane[16:], none], axis=0)
        total = plane + 0.1 * (near_x + near_y + near_z - 6.0 * plane)
        grid_ref[:, k] = total.reshape(16, 16, 128)

    def spread(chunk, slot):
        off_x, off_y, off_z = offsets_of(chunk)
        ids = recv_ids[chunk]
        column = jnp.broadcast_to(ids, (128, 256)).T
        tile_x = jnp.floor(column * 0.0625)
        tile_y = column - 16.0 * tile_x
        placing = onehot(iota((256, 256), 0), ids)
        picks[chunk, 0] = onehot(iota((256, 128), 1), column)
        picks[chunk, 1] = onehot(iota((256, 128), 1) + 128, column)
        x = (recv[chunk, 0:16, :] - (off_x * 16).astype(F32)) * ROOT
        y = (recv[chunk, 16:32, :] - (off_y * 16).astype(F32)) * ROOT
        z = recv[chunk, 32:48, :] - (off_z * 128).astype(F32) - 64.0
        forces = [recv[chunk, 48 + 16 * k : 64 + 16 * k, :] for k in range(3)]
        step = iota((8, 256), 0).astype(F32)
        for r in range(CAP):
            part = slice(r * 16, r * 16 + 16)
            tx = tile_x[part] * ROOT
            ty = tile_y[part] * ROOT
            there = column[part]
            dx = jnp.concatenate([tx, tx], axis=1) - x[r : r + 1]
            dy = jnp.concatenate([ty, ty], axis=1) - y[r : r + 1]
            weight = jnp.exp2(-(dx * dx + dy * dy))
            weight = jnp.where(jnp.concatenate([there, there], axis=1) >= 0.0, weight, 0.0)
            across[chunk, r] = weight
            scaled = jnp.concatenate([(forces[k][r : r + 1] * weight).astype(BF16) for k in range(3)], axis=0)
            dz = step - z[r : r + 1]
            lean = dz * (16.0 * HALF)
            start = dz * dz * HALF
            powers = {8: start}
            up, down = lean + 64.0 * HALF, 64.0 * HALF - lean
            at = start
            for g in range(9, 16):
                at = at + up
                powers[g] = at
                up = up + 128.0 * HALF
            at = start
            for g in range(7, -1, -1):
                at = at + down
                powers[g] = at
                down = down + 128.0 * HALF
            line = jnp.concatenate([jnp.exp2(powers[g]) for g in range(16)], axis=0).astype(BF16)
            along[chunk, r, 0] = line[:, :128]
            along[chunk, r, 1] = line[:, 128:]
            piece = dot_nt(scaled, line).astype(BF16)
            for k in range(3):
                pieces[slot, k, part, :] = piece[16 * k : 16 * k + 16]
        added = dot(placing, jnp.concatenate([pieces[slot, k] for k in range(3)], axis=1))
        for k in range(3):
            grid_ref[:, k] += added[:, 128 * k : 128 * k + 128].reshape(16, 16, 128)

    def spread_pair(chunk):
        spread(chunk, 0)
        spread(chunk + 1, 1)

    @pl.loop(NEAR, CHUNKS, step=2)
    def _(chunk):
        spread_pair(chunk)

    for copy in halos:
        copy.wait()
    at_row0 = (iota((256, CAP), 0) == iota((256, CAP), 1) * CAP).astype(F32)
    at_row15 = (iota((256, CAP), 0) == iota((256, CAP), 1) * CAP + 15).astype(F32)
    for k in range(3):
        grid_ref[0, k] += 0.1 * face_x[0, k]
        grid_ref[15, k] += 0.1 * face_x[1, k]
        extra = jnp.dot(at_row0, face_y[0, k], precision=lax.Precision.HIGHEST, preferred_element_type=F32)
        extra += jnp.dot(at_row15, face_y[1, k], precision=lax.Precision.HIGHEST, preferred_element_type=F32)
        low = jnp.broadcast_to(face_z[0, k : k + 1, :], (128, 256)).T
        high = jnp.broadcast_to(face_z[1, k : k + 1, :], (128, 256)).T
        extra += jnp.where(lane == 0, low, 0.0) + jnp.where(lane == 127, high, 0.0)
        grid_ref[:, k] += 0.1 * extra.reshape(16, 16, 128)

    beside = near((1, 0, 0))

    @pl.loop(0, NEAR, step=2)
    def _(chunk):
        for i in range(2):
            forward_ids(chunk + i, beside).wait_recv()
            forward(chunk + i, beside).wait_recv()
        spread_pair(chunk)

    for k in range(3):
        low_grid[k] = grid_ref[:, k].reshape(256, 128).astype(BF16)

    def sample(chunk, result, slot):
        pick_rows = jnp.concatenate([picks[chunk, 0], picks[chunk, 1]], axis=1)
        u = dot(pick_rows, jnp.concatenate([low_grid[k] for k in range(3)], axis=1)).astype(BF16)
        for k in range(3):
            local_u[slot, :, 16 * k : 16 * k + 16, :] = u[:, 128 * k : 128 * k + 128].reshape(16, 16, 128)
        for half in range(2):
            sums = [[], [], []]
            for r in range(8 * half, 8 * half + 8):
                line = jnp.concatenate([along[chunk, r, 0], along[chunk, r, 1]], axis=1)
                got = dot(local_u[slot, r], line)
                weight = across[chunk, r]
                for k in range(3):
                    value = got[16 * k : 16 * k + 16] * weight
                    sums[k].append(value[0:8] + value[8:16])
            for k in range(3):
                result[k, 8 * half : 8 * half + 8, :] = merged(sums[k])

    def origin(chunk):
        offset = offsets_of(chunk)
        return tuple(lax.rem(me[i] - offset[i] + sizes[i], sizes[i]) for i in range(3))

    @pl.loop(0, NEAR, step=2)
    def _(turn):
        chunk = NEAR - 2 - turn
        for i in range(2):
            sample(chunk + i, ret_send.at[chunk + i], i)
        for i in range(2):
            back(chunk + i, origin(chunk + i)).start()

    @pl.loop(NEAR, CHUNKS, step=2)
    def _(chunk):
        for i in range(2):
            sample(chunk + i, ret_recv.at[chunk + i], i)

    @pl.loop(0, NEAR)
    def _(chunk):
        forward_ids(chunk, beside).wait_send()
        forward(chunk, beside).wait_send()
        back(chunk, beside).wait()

    gather = gather_t[0:64, 0:rows]
    for k in range(3):
        terms = ret_recv[:, k].reshape(rows, 256)
        high = terms.astype(BF16)
        low = (terms - high.astype(F32)).astype(BF16)
        out_ref[k] = dot(gather, high) + dot(gather, low)


def pass_on(grid_in, markers_in, grid_ref, out_ref):
    grid_ref[...] = grid_in[...]
    out_ref[...] = markers_in[...]


def body(sizes, velocity, marker_pos, marker_force, intersect, tiles):
    vmem = pl.BlockSpec(memory_space=pltpu.VMEM)
    dma = pltpu.SemaphoreType.DMA
    grid, markers = pl.pallas_call(
        functools.partial(kernel, sizes),
        out_shape=(
            jax.ShapeDtypeStruct((16, 3, 16, 128), F32),
            jax.ShapeDtypeStruct((3, 64, 256), F32),
        ),
        in_specs=[pl.BlockSpec(memory_space=pl.ANY)] * 5,
        out_specs=(vmem, vmem),
        scratch_shapes=[
            pltpu.VMEM((16, 3, 16, 128), F32),
            pltpu.VMEM((3, 64, 256), F32),
            pltpu.VMEM((3, 64, 256), F32),
            pltpu.VMEM((27, 64), jnp.int32),
            pltpu.VMEM((27, 16, 64), jnp.int32),
            dma((5,)),
            pltpu.VMEM((6, 192, 256), BF16),
            pltpu.VMEM((NEAR, 96, 256), F32),
            pltpu.VMEM((CHUNKS, 96, 256), F32),
            pltpu.VMEM((NEAR, 1, 256), F32),
            pltpu.VMEM((CHUNKS, 1, 256), F32),
            pltpu.VMEM((CHUNKS, CAP, 2, 128, 128), BF16),
            pltpu.VMEM((CHUNKS, CAP, CAP, 256), F32),
            pltpu.VMEM((CHUNKS, 2, 256, 128), BF16),
            pltpu.VMEM((128, 512), BF16),
            pltpu.VMEM((2, 3, 256, 128), BF16),
            pltpu.VMEM((3, 256, 128), BF16),
            pltpu.VMEM((2, CAP, 48, 128), BF16),
            pltpu.VMEM((NEAR, 3, CAP, 256), F32),
            pltpu.VMEM((CHUNKS, 3, CAP, 256), F32),
            pltpu.VMEM((2, 3, CAP, 128), F32),
            pltpu.VMEM((2, 8, 256), F32),
            pltpu.VMEM((2, 3, CAP, 128), F32),
            pltpu.VMEM((2, 3, CAP, 128), F32),
            pltpu.VMEM((2, 8, 256), F32),
            pltpu.SemaphoreType.REGULAR((2,)),
            dma((NEAR,)),
            dma((NEAR,)),
            dma((NEAR,)),
            dma((NEAR,)),
            dma((NEAR,)),
            dma((NEAR,)),
            dma((6,)),
            dma((6,)),
        ],
        compiler_params=pltpu.CompilerParams(
            collective_id=0, has_side_effects=True, vmem_limit_bytes=67043328
        ),
    )(
        jnp.transpose(velocity, (0, 2, 1, 3)),
        jnp.transpose(marker_pos, (1, 0, 2)),
        jnp.transpose(marker_force, (1, 0, 2)),
        intersect.T,
        jnp.transpose(tiles, (1, 2, 0)),
    )
    grid, markers = pl.pallas_call(
        pass_on,
        out_shape=(
            jax.ShapeDtypeStruct((16, 3, 16, 128), F32),
            jax.ShapeDtypeStruct((3, 64, 256), F32),
        ),
        in_specs=[vmem] * 2,
        out_specs=(vmem, vmem),
    )(grid, markers)
    return jnp.transpose(grid, (0, 2, 1, 3)), jnp.transpose(markers, (1, 0, 2))


def solution(mesh):
    sizes = tuple(mesh.shape[name] for name in ("gx", "gy", "gz"))
    placed = (
        P("gx", "gy", None, "gz"),
        P(("gx", "gy", "gz"), None, None),
        P(("gx", "gy", "gz"), None, None),
        P(("gx", "gy", "gz"), None),
        P(("gx", "gy", "gz"), None, None),
    )
    return jax.shard_map(
        functools.partial(body, sizes),
        mesh=mesh,
        in_specs=placed,
        out_specs=(P("gx", "gy", None, "gz"), P(("gx", "gy", "gz"), None, None)),
        check_vma=False,
    )
```

```python
import functools

import jax
import jax.numpy as jnp
from jax import lax
from jax.experimental import pallas as pl
from jax.experimental.pallas import tpu as pltpu
from jax.sharding import PartitionSpec as P

MESH = pl.DeviceIdType.MESH
CAP = 16
NEAR = 26
CHUNKS = 30
LOG2E = 1.4426950408889634
ROOT = (0.5 * LOG2E) ** 0.5
HALF = -0.5 * LOG2E
F32 = jnp.float32
BF16 = jnp.bfloat16


FACES = [(1, 0, 0), (0, 0, 1), (0, 1, 0), (-1, 0, 0), (0, 0, -1), (0, -1, 0)]
EDGES = [
    (1, 0, 1), (0, 1, -1), (-1, 1, 0), (0, -1, 1), (-1, 0, -1), (1, -1, 0),
    (1, 1, 0), (0, -1, -1), (-1, 0, 1), (0, 1, 1), (1, 0, -1), (-1, -1, 0),
]
CORNERS = [
    (1, 1, 1), (-1, -1, -1), (1, -1, 1), (-1, 1, -1), (-1, 1, 1), (1, -1, -1), (1, 1, -1), (-1, -1, 1),
]
ORDER = FACES + EDGES + CORNERS + [(0, 0, 0)] * 4
WORDS = [
    sum((13 + 9 * x + 3 * y + z) << (5 * i) for i, (x, y, z) in enumerate(ORDER[6 * w : 6 * w + 6]))
    for w in range(5)
]


def code_of(chunk):
    word = jnp.where(chunk < 6, WORDS[0], WORDS[1])
    word = jnp.where(chunk < 12, word, WORDS[2])
    word = jnp.where(chunk < 18, word, WORDS[3])
    word = jnp.where(chunk < 24, word, WORDS[4])
    return lax.shift_right_logical(word, 5 * (chunk % 6)) % 32


def offsets_of(chunk):
    code = code_of(chunk)
    return code // 9 - 1, code // 3 % 3 - 1, code % 3 - 1


def iota(shape, dim):
    return lax.broadcasted_iota(jnp.int32, shape, dim)


def dot(a, b):
    return jnp.dot(a, b, preferred_element_type=F32)


def dot_nt(a, b):
    return lax.dot_general(a, b, (((1,), (1,)), ((), ())), preferred_element_type=F32)


def onehot(index, ids):
    return jnp.where(index.astype(F32) == ids, 1.0, 0.0).astype(BF16)


def merged(values):
    row = iota((8, 256), 0)
    for width in (4, 2, 1):
        first = row % (2 * width) < width
        if width == 4:
            values = [
                jnp.where(first, a, b) + pltpu.roll(jnp.where(first, b, a), 4, 0)
                for a, b in zip(values[:4], values[4:])
            ]
        else:
            values = [
                jnp.where(first, a, b) + jnp.where(first, pltpu.roll(a, 8 - width, 0), pltpu.roll(b, width, 0))
                for a, b in zip(values[:width], values[width:])
            ]
    return values[0]


def parts3(value):
    high = value.astype(BF16)
    rest = value - high.astype(F32)
    mid = rest.astype(BF16)
    low = (rest - mid.astype(F32)).astype(BF16)
    return jnp.concatenate([high, mid, low], axis=0)


def kernel(
    sizes, vel_in, pos_in, force_in, flag_in, tile_in, grid_out, out_ref,
    grid_ref, out_sem, vel_ref, pos_ref, force_ref, flag_ref, tile_ref, in_sem, split,
    send, recv, send_ids, recv_ids, along, across, picks, gather_t, pieces, low_grid, local_u, ret_send, ret_recv,
    face_y_send, face_z_send, face_x, face_y, face_z,
    round_sem, send_sem, recv_sem, isend_sem, irecv_sem, rsend_sem, rrecv_sem, hsend_sem, hrecv_sem,
):
    names = ("gx", "gy", "gz")
    me = [lax.axis_index(name) for name in names]
    around = [
        {d: lax.rem(at + (d + size), size) for d in (-1, 0, 1)} for at, size in zip(me, sizes)
    ]

    def near(offset):
        return tuple(around[i][offset[i]] for i in range(3))

    barrier = pltpu.get_barrier_semaphore()
    for face in FACES:
        pl.semaphore_signal(barrier, inc=1, device_id=near(face), device_id_type=MESH)

    loads = [
        pltpu.make_async_copy(source, target, in_sem.at[i])
        for i, (source, target) in enumerate(
            [(flag_in, flag_ref), (pos_in, pos_ref), (force_in, force_ref), (vel_in, vel_ref), (tile_in, tile_ref)]
        )
    ]
    for copy in loads:
        copy.start()

    def halo(index):
        axis, side = divmod(index, 2)
        offset = [0, 0, 0]
        offset[axis] = 1 - 2 * side
        source = (vel_ref.at[15 if side == 0 else 0], face_y_send.at[side], face_z_send.at[side])[axis]
        target = (face_x.at[side], face_y.at[side], face_z.at[side])[axis]
        return pltpu.make_async_remote_copy(
            src_ref=source, dst_ref=target, send_sem=hsend_sem.at[index], recv_sem=hrecv_sem.at[index],
            device_id=near(offset), device_id_type=MESH,
        )

    def forward(n, device):
        return pltpu.make_async_remote_copy(
            src_ref=send.at[n], dst_ref=recv.at[n], send_sem=send_sem.at[n], recv_sem=recv_sem.at[n],
            device_id=device, device_id_type=MESH,
        )

    def forward_ids(n, device):
        return pltpu.make_async_remote_copy(
            src_ref=send_ids.at[n], dst_ref=recv_ids.at[n], send_sem=isend_sem.at[n], recv_sem=irecv_sem.at[n],
            device_id=device, device_id_type=MESH,
        )

    def go(low, high):
        for n in range(low, high):
            forward(n, near(ORDER[n])).start()

    def go_ids(low, high):
        for n in range(low, high):
            forward_ids(n, near(ORDER[n])).start()

    def tell(index):
        for face in FACES:
            pl.semaphore_signal(round_sem.at[index], inc=1, device_id=near(face), device_id_type=MESH)

    def back(n, device):
        return pltpu.make_async_remote_copy(
            src_ref=ret_send.at[n], dst_ref=ret_recv.at[n], send_sem=rsend_sem.at[n], recv_sem=rrecv_sem.at[n],
            device_id=device, device_id_type=MESH,
        )

    loads[0].wait()
    flags = flag_ref[...].astype(F32)
    before = (iota((64, 64), 0) <= iota((64, 64), 1)).astype(F32).astype(BF16)
    ranks = dot(flags.astype(BF16), before) - 1.0
    value = jnp.where(flags > 0.5, ranks, -1.0)
    value = jnp.concatenate([value, value, value], axis=1).astype(BF16)
    lanes27 = iota((CAP, 27), 1)

    def code_rows(low, high):
        return jnp.concatenate(
            [jnp.where(lanes27 == 13 + 9 * x + 3 * y + z, 1.0, 0.0) for x, y, z in ORDER[low:high]], axis=0
        ).astype(BF16)

    def slot_rows(low, high):
        rows = (high - low) * CAP
        slot = (iota((rows, 192), 0) & 15).astype(F32)
        return jnp.where(dot(code_rows(low, high), value) == slot, 1.0, 0.0)

    face_pick = slot_rows(0, 6).astype(BF16)
    loads[1].wait()
    loads[2].wait()
    for f in range(6):
        split[f] = parts3(pos_ref[f] if f < 3 else force_ref[f - 3])
        send[0:6, f * CAP : (f + 1) * CAP, :] = dot(face_pick, split[f]).reshape(6, CAP, 256)

    pl.semaphore_wait(barrier, 6)
    tell(0)
    go(0, 6)

    loads[3].wait()
    last_row = (iota((CAP, 256), 1) == iota((CAP, 256), 0) * CAP + 15).astype(F32)
    first_row = (iota((CAP, 256), 1) == iota((CAP, 256), 0) * CAP).astype(F32)
    z_low, z_high = [], []
    for k in range(3):
        plane = vel_ref[:, k].reshape(256, 128)
        turned = plane.T
        z_low.append(turned[0:1])
        z_high.append(turned[127:128])
        face_y_send[0, k] = jnp.dot(last_row, plane, precision=lax.Precision.HIGHEST, preferred_element_type=F32)
        face_y_send[1, k] = jnp.dot(first_row, plane, precision=lax.Precision.HIGHEST, preferred_element_type=F32)
    pad = [jnp.zeros((5, 256), F32)]
    face_z_send[0] = jnp.concatenate(z_high + pad, axis=0)
    face_z_send[1] = jnp.concatenate(z_low + pad, axis=0)

    rest = slot_rows(6, NEAR)
    rest_pick = rest.astype(BF16)
    own_rows = jnp.where((iota((64, 192), 1) & 63) == iota((64, 192), 0), 1.0, 0.0)
    own_pick = own_rows.astype(BF16)
    for f in range(6):
        got = dot(jnp.concatenate([rest_pick, own_pick], axis=0), split[f]).reshape(CHUNKS - 6, CAP, 256)
        send[6:NEAR, f * CAP : (f + 1) * CAP, :] = got[: NEAR - 6]
        recv[NEAR:, f * CAP : (f + 1) * CAP, :] = got[NEAR - 6 :]
    halos = [halo(i) for i in range(6)]
    for copy in halos:
        copy.start()
    pl.semaphore_wait(round_sem.at[0], 6)
    tell(1)

    loads[4].wait()
    rows = CHUNKS * CAP
    pick = jnp.concatenate([face_pick, rest_pick, own_pick], axis=0)
    ids = (tile_ref[...].reshape(27 * CAP, 64) + 1).astype(F32).astype(BF16)
    all_ids = dot_nt(pick[:, :64], ids)
    each = jnp.where(iota((27, 27 * CAP), 0) == lax.shift_right_logical(iota((27, 27 * CAP), 1), 4), 1.0, 0.0)
    same = dot(code_rows(0, CHUNKS), each.astype(BF16))
    all_ids = (all_ids * same).astype(BF16)
    spread_ids = jnp.where((iota((27 * CAP, 256), 0) & 15) == (iota((27 * CAP, 256), 1) & 15), 1.0, 0.0).astype(BF16)
    wide = dot(all_ids, spread_ids)
    wide = jnp.where((iota((rows, 256), 0) & 15) == lax.shift_right_logical(iota((rows, 256), 1), 4), wide, 0.0)
    id_rows = jnp.sum(wide.reshape(CHUNKS, CAP, 256), axis=1, keepdims=True) - 1.0
    send_ids[...] = id_rows[:NEAR]
    recv_ids[NEAR:] = id_rows[NEAR:]
    go_ids(0, 18)
    go(6, 18)
    face_rows = slot_rows(0, 6)
    gather_t[...] = jnp.concatenate(
        [face_rows[:, :128], rest[:, :128], own_rows[:, :128], jnp.zeros((32, 128), F32)], axis=0
    ).T.astype(BF16)
    pl.semaphore_wait(round_sem.at[1], 6)
    go_ids(18, NEAR)
    go(18, NEAR)

    tile_y = iota((256, 128), 0) % CAP
    lane = iota((256, 128), 1)
    for k in range(3):
        plane = vel_ref[:, k].reshape(256, 128)
        near_y = jnp.where(tile_y == 0, 0.0, pltpu.roll(plane, 1, 0)) + jnp.where(
            tile_y == 15, 0.0, pltpu.roll(plane, 255, 0)
        )
        near_z = jnp.where(lane == 0, 0.0, pltpu.roll(plane, 1, 1)) + jnp.where(
            lane == 127, 0.0, pltpu.roll(plane, 127, 1)
        )
        none = jnp.zeros((CAP, 128), F32)
        near_x = jnp.concatenate([none, plane[:240]], axis=0) + jnp.concatenate([plane[16:], none], axis=0)
        total = plane + 0.1 * (near_x + near_y + near_z - 6.0 * plane)
        grid_ref[:, k] = total.reshape(16, 16, 128)

    def spread(chunk, slot):
        off_x, off_y, off_z = offsets_of(chunk)
        ids = recv_ids[chunk]
        column = jnp.broadcast_to(ids, (128, 256)).T
        tile_x = jnp.floor(column * 0.0625)
        tile_y = column - 16.0 * tile_x
        placing = onehot(iota((256, 256), 0), ids)
        picks[chunk, 0] = onehot(iota((256, 128), 1), column)
        picks[chunk, 1] = onehot(iota((256, 128), 1) + 128, column)
        x = (recv[chunk, 0:16, :] - (off_x * 16).astype(F32)) * ROOT
        y = (recv[chunk, 16:32, :] - (off_y * 16).astype(F32)) * ROOT
        z = recv[chunk, 32:48, :] - (off_z * 128).astype(F32) - 64.0
        forces = [recv[chunk, 48 + 16 * k : 64 + 16 * k, :] for k in range(3)]
        step = iota((8, 256), 0).astype(F32)
        for r in range(CAP):
            part = slice(r * 16, r * 16 + 16)
            tx = tile_x[part] * ROOT
            ty = tile_y[part] * ROOT
            there = column[part]
            dx = jnp.concatenate([tx, tx], axis=1) - x[r : r + 1]
            dy = jnp.concatenate([ty, ty], axis=1) - y[r : r + 1]
            weight = jnp.exp2(-(dx * dx + dy * dy))
            weight = jnp.where(jnp.concatenate([there, there], axis=1) >= 0.0, weight, 0.0)
            across[chunk, r] = weight
            scaled = jnp.concatenate([(forces[k][r : r + 1] * weight).astype(BF16) for k in range(3)], axis=0)
            dz = step - z[r : r + 1]
            lean = dz * (16.0 * HALF)
            start = dz * dz * HALF
            powers = {8: start}
            up, down = lean + 64.0 * HALF, 64.0 * HALF - lean
            at = start
            for g in range(9, 16):
                at = at + up
                powers[g] = at
                up = up + 128.0 * HALF
            at = start
            for g in range(7, -1, -1):
                at = at + down
                powers[g] = at
                down = down + 128.0 * HALF
            line = jnp.concatenate([jnp.exp2(powers[g]) for g in range(16)], axis=0).astype(BF16)
            along[chunk, r, 0] = line[:, :128]
            along[chunk, r, 1] = line[:, 128:]
            piece = dot_nt(scaled, line).astype(BF16)
            for k in range(3):
                pieces[slot, k, part, :] = piece[16 * k : 16 * k + 16]
        added = dot(placing, jnp.concatenate([pieces[slot, k] for k in range(3)], axis=1))
        for k in range(3):
            grid_ref[:, k] += added[:, 128 * k : 128 * k + 128].reshape(16, 16, 128)

    def spread_pair(chunk):
        spread(chunk, 0)
        spread(chunk + 1, 1)

    @pl.loop(NEAR, CHUNKS, step=2)
    def _(chunk):
        spread_pair(chunk)

    for copy in halos:
        copy.wait()
    at_row0 = (iota((256, CAP), 0) == iota((256, CAP), 1) * CAP).astype(F32)
    at_row15 = (iota((256, CAP), 0) == iota((256, CAP), 1) * CAP + 15).astype(F32)
    for k in range(3):
        grid_ref[0, k] += 0.1 * face_x[0, k]
        grid_ref[15, k] += 0.1 * face_x[1, k]
        extra = jnp.dot(at_row0, face_y[0, k], precision=lax.Precision.HIGHEST, preferred_element_type=F32)
        extra += jnp.dot(at_row15, face_y[1, k], precision=lax.Precision.HIGHEST, preferred_element_type=F32)
        low = jnp.broadcast_to(face_z[0, k : k + 1, :], (128, 256)).T
        high = jnp.broadcast_to(face_z[1, k : k + 1, :], (128, 256)).T
        extra += jnp.where(lane == 0, low, 0.0) + jnp.where(lane == 127, high, 0.0)
        grid_ref[:, k] += 0.1 * extra.reshape(16, 16, 128)

    beside = near((1, 0, 0))

    @pl.loop(0, NEAR, step=2)
    def _(chunk):
        for i in range(2):
            forward_ids(chunk + i, beside).wait_recv()
            forward(chunk + i, beside).wait_recv()
        spread_pair(chunk)

    for k in range(3):
        low_grid[k] = grid_ref[:, k].reshape(256, 128).astype(BF16)

    grid_copy = pltpu.make_async_copy(grid_ref, grid_out, out_sem)
    grid_copy.start()

    def fetch(chunk):
        pick_rows = jnp.concatenate(
            [jnp.concatenate([picks[chunk + i, 0], picks[chunk + i, 1]], axis=1) for i in range(2)], axis=0
        )
        u = dot(pick_rows, jnp.concatenate([low_grid[k] for k in range(3)], axis=1)).astype(BF16)
        for k in range(3):
            local_u[:, :, 16 * k : 16 * k + 16, :] = u[:, 128 * k : 128 * k + 128].reshape(2, 16, 16, 128)

    def sample(chunk, result, slot):
        for half in range(2):
            sums = [[], [], []]
            for r in range(8 * half, 8 * half + 8):
                line = jnp.concatenate([along[chunk, r, 0], along[chunk, r, 1]], axis=1)
                got = dot(local_u[slot, r], line)
                weight = across[chunk, r]
                for k in range(3):
                    value = got[16 * k : 16 * k + 16] * weight
                    sums[k].append(value[0:8] + value[8:16])
            for k in range(3):
                result[k, 8 * half : 8 * half + 8, :] = merged(sums[k])

    def origin(chunk):
        offset = offsets_of(chunk)
        return tuple(lax.rem(me[i] - offset[i] + sizes[i], sizes[i]) for i in range(3))

    @pl.loop(0, NEAR, step=2)
    def _(turn):
        chunk = NEAR - 2 - turn
        fetch(chunk)
        for i in range(2):
            sample(chunk + i, ret_send.at[chunk + i], i)
        for i in range(2):
            back(chunk + i, origin(chunk + i)).start()

    @pl.loop(NEAR, CHUNKS, step=2)
    def _(chunk):
        fetch(chunk)
        for i in range(2):
            sample(chunk + i, ret_recv.at[chunk + i], i)

    @pl.loop(0, NEAR)
    def _(chunk):
        forward_ids(chunk, beside).wait_send()
        forward(chunk, beside).wait_send()

    def take(low, high):
        gather = gather_t[0:64, low * CAP : high * CAP]
        result = []
        for k in range(3):
            terms = ret_recv[low:high, k].reshape((high - low) * CAP, 256)
            top = terms.astype(BF16)
            rest_part = (terms - top.astype(F32)).astype(BF16)
            result.append(dot(gather, top) + dot(gather, rest_part))
        return result

    @pl.loop(8, NEAR)
    def _(chunk):
        back(chunk, beside).wait()

    early = take(8, CHUNKS)
    for k in range(3):
        out_ref[k] = early[k]

    @pl.loop(0, 8)
    def _(chunk):
        back(chunk, beside).wait()

    late = take(0, 8)
    for k in range(3):
        out_ref[k] += late[k]
    grid_copy.wait()


def pass_on(grid_in, markers_in, grid_out, markers_out, grid, markers, in_sem, out_sem):
    pieces = [(grid_in.at[4 * i : 4 * i + 4], grid.at[4 * i : 4 * i + 4], grid_out.at[4 * i : 4 * i + 4]) for i in range(4)]
    pieces += [(markers_in.at[k], markers.at[k], markers_out.at[k]) for k in range(3)]
    loads = [pltpu.make_async_copy(a, b, in_sem.at[i]) for i, (a, b, _) in enumerate(pieces)]
    stores = [pltpu.make_async_copy(b, c, out_sem.at[i]) for i, (_, b, c) in enumerate(pieces)]
    for load in loads:
        load.start()
    for load, store in zip(loads, stores):
        load.wait()
        store.start()
    for store in stores:
        store.wait()


def body(sizes, velocity, marker_pos, marker_force, intersect, tiles):
    vmem = pl.BlockSpec(memory_space=pltpu.VMEM)
    dma = pltpu.SemaphoreType.DMA
    grid, markers = pl.pallas_call(
        functools.partial(kernel, sizes),
        out_shape=(
            jax.ShapeDtypeStruct((16, 3, 16, 128), F32),
            jax.ShapeDtypeStruct((3, 64, 256), F32),
        ),
        in_specs=[pl.BlockSpec(memory_space=pl.ANY)] * 5,
        out_specs=(pl.BlockSpec(memory_space=pl.ANY), vmem),
        scratch_shapes=[
            pltpu.VMEM((16, 3, 16, 128), F32),
            pltpu.SemaphoreType.DMA,
            pltpu.VMEM((16, 3, 16, 128), F32),
            pltpu.VMEM((3, 64, 256), F32),
            pltpu.VMEM((3, 64, 256), F32),
            pltpu.VMEM((27, 64), jnp.int32),
            pltpu.VMEM((27, 16, 64), jnp.int32),
            dma((5,)),
            pltpu.VMEM((6, 192, 256), BF16),
            pltpu.VMEM((NEAR, 96, 256), F32),
            pltpu.VMEM((CHUNKS, 96, 256), F32),
            pltpu.VMEM((NEAR, 1, 256), F32),
            pltpu.VMEM((CHUNKS, 1, 256), F32),
            pltpu.VMEM((CHUNKS, CAP, 2, 128, 128), BF16),
            pltpu.VMEM((CHUNKS, CAP, CAP, 256), F32),
            pltpu.VMEM((CHUNKS, 2, 256, 128), BF16),
            pltpu.VMEM((128, 512), BF16),
            pltpu.VMEM((2, 3, 256, 128), BF16),
            pltpu.VMEM((3, 256, 128), BF16),
            pltpu.VMEM((2, CAP, 48, 128), BF16),
            pltpu.VMEM((NEAR, 3, CAP, 256), F32),
            pltpu.VMEM((CHUNKS, 3, CAP, 256), F32),
            pltpu.VMEM((2, 3, CAP, 128), F32),
            pltpu.VMEM((2, 8, 256), F32),
            pltpu.VMEM((2, 3, CAP, 128), F32),
            pltpu.VMEM((2, 3, CAP, 128), F32),
            pltpu.VMEM((2, 8, 256), F32),
            pltpu.SemaphoreType.REGULAR((2,)),
            dma((NEAR,)),
            dma((NEAR,)),
            dma((NEAR,)),
            dma((NEAR,)),
            dma((NEAR,)),
            dma((NEAR,)),
            dma((6,)),
            dma((6,)),
        ],
        compiler_params=pltpu.CompilerParams(
            collective_id=0, has_side_effects=True, vmem_limit_bytes=67043328
        ),
    )(
        jnp.transpose(velocity, (0, 2, 1, 3)),
        jnp.transpose(marker_pos, (1, 0, 2)),
        jnp.transpose(marker_force, (1, 0, 2)),
        intersect.T,
        jnp.transpose(tiles, (1, 2, 0)),
    )
    grid, markers = pl.pallas_call(
        pass_on,
        out_shape=(
            jax.ShapeDtypeStruct((16, 3, 16, 128), F32),
            jax.ShapeDtypeStruct((3, 64, 256), F32),
        ),
        in_specs=[pl.BlockSpec(memory_space=pl.ANY)] * 2,
        out_specs=(pl.BlockSpec(memory_space=pl.ANY), pl.BlockSpec(memory_space=pl.ANY)),
        scratch_shapes=[
            pltpu.VMEM((16, 3, 16, 128), F32),
            pltpu.VMEM((3, 64, 256), F32),
            dma((7,)),
            dma((7,)),
        ],
    )(grid, markers)
    return jnp.transpose(grid, (0, 2, 1, 3)), jnp.transpose(markers, (1, 0, 2))


def solution(mesh):
    sizes = tuple(mesh.shape[name] for name in ("gx", "gy", "gz"))
    placed = (
        P("gx", "gy", None, "gz"),
        P(("gx", "gy", "gz"), None, None),
        P(("gx", "gy", "gz"), None, None),
        P(("gx", "gy", "gz"), None),
        P(("gx", "gy", "gz"), None, None),
    )
    return jax.shard_map(
        functools.partial(body, sizes),
        mesh=mesh,
        in_specs=placed,
        out_specs=(P("gx", "gy", None, "gz"), P(("gx", "gy", "gz"), None, None)),
        check_vma=False,
    )
```

```python
import functools

import jax
import jax.numpy as jnp
from jax import lax
from jax.experimental import pallas as pl
from jax.experimental.pallas import tpu as pltpu
from jax.sharding import PartitionSpec as P

MESH = pl.DeviceIdType.MESH
CAP = 16
NEAR = 26
CHUNKS = 30
LOG2E = 1.4426950408889634
ROOT = (0.5 * LOG2E) ** 0.5
HALF = -0.5 * LOG2E
F32 = jnp.float32
BF16 = jnp.bfloat16


FACES = [(1, 0, 0), (0, 0, 1), (0, 1, 0), (-1, 0, 0), (0, 0, -1), (0, -1, 0)]
EDGES = [(0, 1, 1), (0, -1, -1), (0, 1, -1), (0, -1, 1), (1, 0, 1), (-1, 1, 0), (-1, 0, -1), (1, -1, 0), (-1, 0, 1), (1, 1, 0), (1, 0, -1), (-1, -1, 0)]
CORNERS = [
    (1, 1, 1), (-1, -1, -1), (1, -1, 1), (-1, 1, -1), (-1, 1, 1), (1, -1, -1), (1, 1, -1), (-1, -1, 1),
]
ORDER = FACES + EDGES + CORNERS + [(0, 0, 0)] * 4
WORDS = [
    sum((13 + 9 * x + 3 * y + z) << (5 * i) for i, (x, y, z) in enumerate(ORDER[6 * w : 6 * w + 6]))
    for w in range(5)
]


def code_of(chunk):
    word = jnp.where(chunk < 6, WORDS[0], WORDS[1])
    word = jnp.where(chunk < 12, word, WORDS[2])
    word = jnp.where(chunk < 18, word, WORDS[3])
    word = jnp.where(chunk < 24, word, WORDS[4])
    return lax.shift_right_logical(word, 5 * (chunk % 6)) % 32


def offsets_of(chunk):
    code = code_of(chunk)
    return code // 9 - 1, code // 3 % 3 - 1, code % 3 - 1


def iota(shape, dim):
    return lax.broadcasted_iota(jnp.int32, shape, dim)


def dot(a, b):
    return jnp.dot(a, b, preferred_element_type=F32)


def dot_nt(a, b):
    return lax.dot_general(a, b, (((1,), (1,)), ((), ())), preferred_element_type=F32)


def onehot(index, ids):
    return jnp.where(index.astype(F32) == ids, 1.0, 0.0).astype(BF16)


def merged(values):
    row = iota((8, 256), 0)
    for width in (4, 2, 1):
        first = row % (2 * width) < width
        if width == 4:
            values = [
                jnp.where(first, a, b) + pltpu.roll(jnp.where(first, b, a), 4, 0)
                for a, b in zip(values[:4], values[4:])
            ]
        else:
            values = [
                jnp.where(first, a, b) + jnp.where(first, pltpu.roll(a, 8 - width, 0), pltpu.roll(b, width, 0))
                for a, b in zip(values[:width], values[width:])
            ]
    return values[0]


def parts3(value):
    high = value.astype(BF16)
    rest = value - high.astype(F32)
    mid = rest.astype(BF16)
    low = (rest - mid.astype(F32)).astype(BF16)
    return jnp.concatenate([high, mid, low], axis=0)


def kernel(
    sizes, vel_in, pos_in, force_in, flag_in, tile_in, grid_out, out_ref,
    grid_ref, out_sem, vel_ref, pos_ref, force_ref, flag_ref, tile_ref, in_sem, split,
    send, recv, send_ids, recv_ids, along, across, picks, gather_t, pieces, low_grid, local_u, ret_send, ret_recv,
    face_y_send, face_z_send, face_x, face_y, face_z,
    round_sem, send_sem, recv_sem, isend_sem, irecv_sem, rsend_sem, rrecv_sem, hsend_sem, hrecv_sem,
):
    names = ("gx", "gy", "gz")
    me = [lax.axis_index(name) for name in names]
    around = [
        {d: lax.rem(at + (d + size), size) for d in (-1, 0, 1)} for at, size in zip(me, sizes)
    ]

    def near(offset):
        return tuple(around[i][offset[i]] for i in range(3))

    barrier = pltpu.get_barrier_semaphore()
    for face in FACES:
        pl.semaphore_signal(barrier, inc=1, device_id=near(face), device_id_type=MESH)

    loads = [
        pltpu.make_async_copy(source, target, in_sem.at[i])
        for i, (source, target) in enumerate(
            [(flag_in, flag_ref), (pos_in, pos_ref), (force_in, force_ref), (vel_in, vel_ref), (tile_in, tile_ref)]
        )
    ]
    for copy in loads:
        copy.start()

    def halo(index):
        axis, side = divmod(index, 2)
        offset = [0, 0, 0]
        offset[axis] = 1 - 2 * side
        source = (vel_ref.at[15 if side == 0 else 0], face_y_send.at[side], face_z_send.at[side])[axis]
        target = (face_x.at[side], face_y.at[side], face_z.at[side])[axis]
        return pltpu.make_async_remote_copy(
            src_ref=source, dst_ref=target, send_sem=hsend_sem.at[index], recv_sem=hrecv_sem.at[index],
            device_id=near(offset), device_id_type=MESH,
        )

    def forward(n, device):
        return pltpu.make_async_remote_copy(
            src_ref=send.at[n], dst_ref=recv.at[n], send_sem=send_sem.at[n], recv_sem=recv_sem.at[n],
            device_id=device, device_id_type=MESH,
        )

    def forward_ids(n, device):
        return pltpu.make_async_remote_copy(
            src_ref=send_ids.at[n], dst_ref=recv_ids.at[n], send_sem=isend_sem.at[n], recv_sem=irecv_sem.at[n],
            device_id=device, device_id_type=MESH,
        )

    def go(low, high):
        for n in range(low, high):
            forward(n, near(ORDER[n])).start()

    def go_ids(low, high):
        for n in range(low, high):
            forward_ids(n, near(ORDER[n])).start()

    def tell(index):
        for face in FACES:
            pl.semaphore_signal(round_sem.at[index], inc=1, device_id=near(face), device_id_type=MESH)

    def back(n, device):
        return pltpu.make_async_remote_copy(
            src_ref=ret_send.at[n], dst_ref=ret_recv.at[n], send_sem=rsend_sem.at[n], recv_sem=rrecv_sem.at[n],
            device_id=device, device_id_type=MESH,
        )

    loads[0].wait()
    flags = flag_ref[...].astype(F32)
    before = (iota((64, 64), 0) <= iota((64, 64), 1)).astype(F32).astype(BF16)
    ranks = dot(flags.astype(BF16), before) - 1.0
    value = jnp.where(flags > 0.5, ranks, -1.0)
    value = jnp.concatenate([value, value, value], axis=1).astype(BF16)
    lanes27 = iota((CAP, 27), 1)

    def code_rows(low, high):
        return jnp.concatenate(
            [jnp.where(lanes27 == 13 + 9 * x + 3 * y + z, 1.0, 0.0) for x, y, z in ORDER[low:high]], axis=0
        ).astype(BF16)

    def slot_rows(low, high):
        rows = (high - low) * CAP
        slot = (iota((rows, 192), 0) & 15).astype(F32)
        return jnp.where(dot(code_rows(low, high), value) == slot, 1.0, 0.0)

    face_pick = slot_rows(0, 6).astype(BF16)
    loads[1].wait()
    loads[2].wait()
    for f in range(6):
        split[f] = parts3(pos_ref[f] if f < 3 else force_ref[f - 3])
        send[0:6, f * CAP : (f + 1) * CAP, :] = dot(face_pick, split[f]).reshape(6, CAP, 256)

    pl.semaphore_wait(barrier, 6)
    tell(0)
    go(0, 6)

    loads[3].wait()
    last_row = (iota((CAP, 256), 1) == iota((CAP, 256), 0) * CAP + 15).astype(F32)
    first_row = (iota((CAP, 256), 1) == iota((CAP, 256), 0) * CAP).astype(F32)
    z_low, z_high = [], []
    for k in range(3):
        plane = vel_ref[:, k].reshape(256, 128)
        turned = plane.T
        z_low.append(turned[0:1])
        z_high.append(turned[127:128])
        face_y_send[0, k] = jnp.dot(last_row, plane, precision=lax.Precision.HIGHEST, preferred_element_type=F32)
        face_y_send[1, k] = jnp.dot(first_row, plane, precision=lax.Precision.HIGHEST, preferred_element_type=F32)
    pad = [jnp.zeros((5, 256), F32)]
    face_z_send[0] = jnp.concatenate(z_high + pad, axis=0)
    face_z_send[1] = jnp.concatenate(z_low + pad, axis=0)

    rest = slot_rows(6, NEAR)
    rest_pick = rest.astype(BF16)
    own_rows = jnp.where((iota((64, 192), 1) & 63) == iota((64, 192), 0), 1.0, 0.0)
    own_pick = own_rows.astype(BF16)
    for f in range(6):
        got = dot(jnp.concatenate([rest_pick, own_pick], axis=0), split[f]).reshape(CHUNKS - 6, CAP, 256)
        send[6:NEAR, f * CAP : (f + 1) * CAP, :] = got[: NEAR - 6]
        recv[NEAR:, f * CAP : (f + 1) * CAP, :] = got[NEAR - 6 :]
    halos = [halo(i) for i in range(6)]
    for copy in halos:
        copy.start()
    pl.semaphore_wait(round_sem.at[0], 6)
    tell(1)

    loads[4].wait()
    rows = CHUNKS * CAP
    pick = jnp.concatenate([face_pick, rest_pick, own_pick], axis=0)
    ids = (tile_ref[...].reshape(27 * CAP, 64) + 1).astype(F32).astype(BF16)
    all_ids = dot_nt(pick[:, :64], ids)
    each = jnp.where(iota((27, 27 * CAP), 0) == lax.shift_right_logical(iota((27, 27 * CAP), 1), 4), 1.0, 0.0)
    same = dot(code_rows(0, CHUNKS), each.astype(BF16))
    all_ids = (all_ids * same).astype(BF16)
    spread_ids = jnp.where((iota((27 * CAP, 256), 0) & 15) == (iota((27 * CAP, 256), 1) & 15), 1.0, 0.0).astype(BF16)
    wide = dot(all_ids, spread_ids)
    wide = jnp.where((iota((rows, 256), 0) & 15) == lax.shift_right_logical(iota((rows, 256), 1), 4), wide, 0.0)
    id_rows = jnp.sum(wide.reshape(CHUNKS, CAP, 256), axis=1, keepdims=True) - 1.0
    send_ids[...] = id_rows[:NEAR]
    recv_ids[NEAR:] = id_rows[NEAR:]
    go_ids(0, 18)
    go(6, 18)
    face_rows = slot_rows(0, 6)
    gather_t[...] = jnp.concatenate(
        [face_rows[:, :128], rest[:, :128], own_rows[:, :128], jnp.zeros((32, 128), F32)], axis=0
    ).T.astype(BF16)
    pl.semaphore_wait(round_sem.at[1], 6)
    go_ids(18, NEAR)
    go(18, NEAR)

    tile_y = iota((256, 128), 0) % CAP
    lane = iota((256, 128), 1)
    for k in range(3):
        plane = vel_ref[:, k].reshape(256, 128)
        near_y = jnp.where(tile_y == 0, 0.0, pltpu.roll(plane, 1, 0)) + jnp.where(
            tile_y == 15, 0.0, pltpu.roll(plane, 255, 0)
        )
        near_z = jnp.where(lane == 0, 0.0, pltpu.roll(plane, 1, 1)) + jnp.where(
            lane == 127, 0.0, pltpu.roll(plane, 127, 1)
        )
        none = jnp.zeros((CAP, 128), F32)
        near_x = jnp.concatenate([none, plane[:240]], axis=0) + jnp.concatenate([plane[16:], none], axis=0)
        total = plane + 0.1 * (near_x + near_y + near_z - 6.0 * plane)
        grid_ref[:, k] = total.reshape(16, 16, 128)

    def spread(chunk, slot):
        off_x, off_y, off_z = offsets_of(chunk)
        ids = recv_ids[chunk]
        column = jnp.broadcast_to(ids, (128, 256)).T
        tile_x = jnp.floor(column * 0.0625)
        tile_y = column - 16.0 * tile_x
        placing = onehot(iota((256, 256), 0), ids)
        picks[chunk, 0] = onehot(iota((256, 128), 1), column)
        picks[chunk, 1] = onehot(iota((256, 128), 1) + 128, column)
        x = (recv[chunk, 0:16, :] - (off_x * 16).astype(F32)) * ROOT
        y = (recv[chunk, 16:32, :] - (off_y * 16).astype(F32)) * ROOT
        z = recv[chunk, 32:48, :] - (off_z * 128).astype(F32) - 64.0
        forces = [recv[chunk, 48 + 16 * k : 64 + 16 * k, :] for k in range(3)]
        step = iota((8, 256), 0).astype(F32)
        for r in range(CAP):
            part = slice(r * 16, r * 16 + 16)
            tx = tile_x[part] * ROOT
            ty = tile_y[part] * ROOT
            there = column[part]
            dx = jnp.concatenate([tx, tx], axis=1) - x[r : r + 1]
            dy = jnp.concatenate([ty, ty], axis=1) - y[r : r + 1]
            weight = jnp.exp2(-(dx * dx + dy * dy))
            weight = jnp.where(jnp.concatenate([there, there], axis=1) >= 0.0, weight, 0.0)
            across[chunk, r] = weight
            scaled = jnp.concatenate([(forces[k][r : r + 1] * weight).astype(BF16) for k in range(3)], axis=0)
            dz = step - z[r : r + 1]
            lean = dz * (16.0 * HALF)
            start = dz * dz * HALF
            powers = {8: start}
            up, down = lean + 64.0 * HALF, 64.0 * HALF - lean
            at = start
            for g in range(9, 16):
                at = at + up
                powers[g] = at
                up = up + 128.0 * HALF
            at = start
            for g in range(7, -1, -1):
                at = at + down
                powers[g] = at
                down = down + 128.0 * HALF
            line = jnp.concatenate([jnp.exp2(powers[g]) for g in range(16)], axis=0).astype(BF16)
            along[chunk, r, 0] = line[:, :128]
            along[chunk, r, 1] = line[:, 128:]
            piece = dot_nt(scaled, line).astype(BF16)
            for k in range(3):
                pieces[slot, k, part, :] = piece[16 * k : 16 * k + 16]
        added = dot(placing, jnp.concatenate([pieces[slot, k] for k in range(3)], axis=1))
        for k in range(3):
            grid_ref[:, k] += added[:, 128 * k : 128 * k + 128].reshape(16, 16, 128)

    def spread_pair(chunk):
        spread(chunk, 0)
        spread(chunk + 1, 1)

    @pl.loop(NEAR, CHUNKS, step=2)
    def _(chunk):
        spread_pair(chunk)

    for copy in halos:
        copy.wait()
    at_row0 = (iota((256, CAP), 0) == iota((256, CAP), 1) * CAP).astype(F32)
    at_row15 = (iota((256, CAP), 0) == iota((256, CAP), 1) * CAP + 15).astype(F32)
    for k in range(3):
        grid_ref[0, k] += 0.1 * face_x[0, k]
        grid_ref[15, k] += 0.1 * face_x[1, k]
        extra = jnp.dot(at_row0, face_y[0, k], precision=lax.Precision.HIGHEST, preferred_element_type=F32)
        extra += jnp.dot(at_row15, face_y[1, k], precision=lax.Precision.HIGHEST, preferred_element_type=F32)
        low = jnp.broadcast_to(face_z[0, k : k + 1, :], (128, 256)).T
        high = jnp.broadcast_to(face_z[1, k : k + 1, :], (128, 256)).T
        extra += jnp.where(lane == 0, low, 0.0) + jnp.where(lane == 127, high, 0.0)
        grid_ref[:, k] += 0.1 * extra.reshape(16, 16, 128)

    beside = near((1, 0, 0))

    @pl.loop(0, NEAR, step=2)
    def _(chunk):
        for i in range(2):
            forward_ids(chunk + i, beside).wait_recv()
            forward(chunk + i, beside).wait_recv()
        spread_pair(chunk)

    for k in range(3):
        low_grid[k] = grid_ref[:, k].reshape(256, 128).astype(BF16)

    grid_copy = pltpu.make_async_copy(grid_ref, grid_out, out_sem)
    grid_copy.start()

    def fetch(chunk):
        pick_rows = jnp.concatenate(
            [jnp.concatenate([picks[chunk + i, 0], picks[chunk + i, 1]], axis=1) for i in range(2)], axis=0
        )
        u = dot(pick_rows, jnp.concatenate([low_grid[k] for k in range(3)], axis=1)).astype(BF16)
        for k in range(3):
            local_u[:, :, 16 * k : 16 * k + 16, :] = u[:, 128 * k : 128 * k + 128].reshape(2, 16, 16, 128)

    def sample(chunk, result, slot):
        for half in range(2):
            sums = [[], [], []]
            for r in range(8 * half, 8 * half + 8):
                line = jnp.concatenate([along[chunk, r, 0], along[chunk, r, 1]], axis=1)
                got = dot(local_u[slot, r], line)
                weight = across[chunk, r]
                for k in range(3):
                    value = got[16 * k : 16 * k + 16] * weight
                    sums[k].append(value[0:8] + value[8:16])
            for k in range(3):
                result[k, 8 * half : 8 * half + 8, :] = merged(sums[k])

    def origin(chunk):
        offset = offsets_of(chunk)
        return tuple(lax.rem(me[i] - offset[i] + sizes[i], sizes[i]) for i in range(3))

    @pl.loop(0, NEAR, step=2)
    def _(turn):
        chunk = NEAR - 2 - turn
        fetch(chunk)
        for i in range(2):
            sample(chunk + i, ret_send.at[chunk + i], i)
        for i in range(2):
            back(chunk + i, origin(chunk + i)).start()

    @pl.loop(NEAR, CHUNKS, step=2)
    def _(chunk):
        fetch(chunk)
        for i in range(2):
            sample(chunk + i, ret_recv.at[chunk + i], i)

    @pl.loop(0, NEAR)
    def _(chunk):
        forward_ids(chunk, beside).wait_send()
        forward(chunk, beside).wait_send()

    def take(low, high):
        gather = gather_t[0:64, low * CAP : high * CAP]
        result = []
        for k in range(3):
            terms = ret_recv[low:high, k].reshape((high - low) * CAP, 256)
            top = terms.astype(BF16)
            rest_part = (terms - top.astype(F32)).astype(BF16)
            result.append(dot(gather, top) + dot(gather, rest_part))
        return result

    @pl.loop(8, NEAR)
    def _(chunk):
        back(chunk, beside).wait()

    early = take(8, CHUNKS)
    for k in range(3):
        out_ref[k] = early[k]

    @pl.loop(0, 8)
    def _(chunk):
        back(chunk, beside).wait()

    late = take(0, 8)
    for k in range(3):
        out_ref[k] += late[k]
    grid_copy.wait()


def pass_on(grid_in, markers_in, grid_out, markers_out, grid, markers, in_sem, out_sem):
    pieces = [(grid_in.at[4 * i : 4 * i + 4], grid.at[4 * i : 4 * i + 4], grid_out.at[4 * i : 4 * i + 4]) for i in range(4)]
    pieces += [(markers_in.at[k], markers.at[k], markers_out.at[k]) for k in range(3)]
    loads = [pltpu.make_async_copy(a, b, in_sem.at[i]) for i, (a, b, _) in enumerate(pieces)]
    stores = [pltpu.make_async_copy(b, c, out_sem.at[i]) for i, (_, b, c) in enumerate(pieces)]
    for load in loads:
        load.start()
    for load, store in zip(loads, stores):
        load.wait()
        store.start()
    for store in stores:
        store.wait()


def body(sizes, velocity, marker_pos, marker_force, intersect, tiles):
    vmem = pl.BlockSpec(memory_space=pltpu.VMEM)
    dma = pltpu.SemaphoreType.DMA
    grid, markers = pl.pallas_call(
        functools.partial(kernel, sizes),
        out_shape=(
            jax.ShapeDtypeStruct((16, 3, 16, 128), F32),
            jax.ShapeDtypeStruct((3, 64, 256), F32),
        ),
        in_specs=[pl.BlockSpec(memory_space=pl.ANY)] * 5,
        out_specs=(pl.BlockSpec(memory_space=pl.ANY), vmem),
        scratch_shapes=[
            pltpu.VMEM((16, 3, 16, 128), F32),
            pltpu.SemaphoreType.DMA,
            pltpu.VMEM((16, 3, 16, 128), F32),
            pltpu.VMEM((3, 64, 256), F32),
            pltpu.VMEM((3, 64, 256), F32),
            pltpu.VMEM((27, 64), jnp.int32),
            pltpu.VMEM((27, 16, 64), jnp.int32),
            dma((5,)),
            pltpu.VMEM((6, 192, 256), BF16),
            pltpu.VMEM((NEAR, 96, 256), F32),
            pltpu.VMEM((CHUNKS, 96, 256), F32),
            pltpu.VMEM((NEAR, 1, 256), F32),
            pltpu.VMEM((CHUNKS, 1, 256), F32),
            pltpu.VMEM((CHUNKS, CAP, 2, 128, 128), BF16),
            pltpu.VMEM((CHUNKS, CAP, CAP, 256), F32),
            pltpu.VMEM((CHUNKS, 2, 256, 128), BF16),
            pltpu.VMEM((128, 512), BF16),
            pltpu.VMEM((2, 3, 256, 128), BF16),
            pltpu.VMEM((3, 256, 128), BF16),
            pltpu.VMEM((2, CAP, 48, 128), BF16),
            pltpu.VMEM((NEAR, 3, CAP, 256), F32),
            pltpu.VMEM((CHUNKS, 3, CAP, 256), F32),
            pltpu.VMEM((2, 3, CAP, 128), F32),
            pltpu.VMEM((2, 8, 256), F32),
            pltpu.VMEM((2, 3, CAP, 128), F32),
            pltpu.VMEM((2, 3, CAP, 128), F32),
            pltpu.VMEM((2, 8, 256), F32),
            pltpu.SemaphoreType.REGULAR((2,)),
            dma((NEAR,)),
            dma((NEAR,)),
            dma((NEAR,)),
            dma((NEAR,)),
            dma((NEAR,)),
            dma((NEAR,)),
            dma((6,)),
            dma((6,)),
        ],
        compiler_params=pltpu.CompilerParams(
            collective_id=0, has_side_effects=True, vmem_limit_bytes=67043328
        ),
    )(
        jnp.transpose(velocity, (0, 2, 1, 3)),
        jnp.transpose(marker_pos, (1, 0, 2)),
        jnp.transpose(marker_force, (1, 0, 2)),
        intersect.T,
        jnp.transpose(tiles, (1, 2, 0)),
    )
    grid, markers = pl.pallas_call(
        pass_on,
        out_shape=(
            jax.ShapeDtypeStruct((16, 3, 16, 128), F32),
            jax.ShapeDtypeStruct((3, 64, 256), F32),
        ),
        in_specs=[pl.BlockSpec(memory_space=pl.ANY)] * 2,
        out_specs=(pl.BlockSpec(memory_space=pl.ANY), pl.BlockSpec(memory_space=pl.ANY)),
        scratch_shapes=[
            pltpu.VMEM((16, 3, 16, 128), F32),
            pltpu.VMEM((3, 64, 256), F32),
            dma((7,)),
            dma((7,)),
        ],
    )(grid, markers)
    return jnp.transpose(grid, (0, 2, 1, 3)), jnp.transpose(markers, (1, 0, 2))


def solution(mesh):
    sizes = tuple(mesh.shape[name] for name in ("gx", "gy", "gz"))
    placed = (
        P("gx", "gy", None, "gz"),
        P(("gx", "gy", "gz"), None, None),
        P(("gx", "gy", "gz"), None, None),
        P(("gx", "gy", "gz"), None),
        P(("gx", "gy", "gz"), None, None),
    )
    return jax.shard_map(
        functools.partial(body, sizes),
        mesh=mesh,
        in_specs=placed,
        out_specs=(P("gx", "gy", None, "gz"), P(("gx", "gy", "gz"), None, None)),
        check_vma=False,
    )
```
